32 devices in a mesh: gx: 8 (over z, x), gy: 4 (over y, core).
Axes of the slice: x: 2, y: 2, z: 4, core: 2. Of those that a mesh axis runs over, the one named last changes fastest.
Arguments:
- measures: bfloat16 [262144, 128], P(('gx', 'gy')), may hold values from -6 to 6
- row_keys: int32 [262144], P(('gx', 'gy')), may hold values from 0 to 16383, as said below
- orders: bfloat16 [16384, 128], P(('gx', 'gy')), may hold values from -6 to 6
- heavy_keys: int32 [64], replicated, may hold values from 0 to 16383, as said below
- key_slot: int32 [16384], replicated, may hold values from 0 to 16383, as said below
Outputs:
- result: bfloat16 [16384, 128], P(('gx', 'gy'))
- heavy_report: bfloat16 [64, 128], P(('gx', 'gy'))
- slot_rows: float32 [16384], P(('gx', 'gy'))
The draws below stay inside these ranges and needn't reach their ends.
Inputs may be any that keep to these rules, and one draw needn't show every extreme that they name: `heavy_keys`: for each range block d, entries d * 2 to (d + 1) * 2 - 1 are distinct keys of d * 512 to (d + 1) * 512 - 1. `key_slot`: A permutation. Slot s belongs to owner s // 2048 and to quarter (s // 512) % q with q = 4. Key k lies in range block d = k // 512; every range block has exactly 64 keys with slots of each owner, all in quarter d % q. `row_keys`: in the rows of one device, among rows whose key is not heavy, at most 768 have slots of any one owner and at most 192 distinct keys have slots of any one owner; in every device both bounds are reached by some owner.
All inputs are finite; a program needn't handle non-finite values.
Results may differ from the reference program's by a relative error of at most 0.0021.
Values may be sent and summed in bfloat16 or wider, within the bound.
A program may use at most 64 MiB of HBM per device.

```python
import jax
import jax.numpy as jnp
from jax import lax

W = 128
ROWS_DEV = 8192
KEY_DEV = 512
HPD = 2
ROWS = 262144
KEYS = 16384
HEAVY = 64
OWN_SLOTS = 2048
KPP = 64
CAP = 768
CAPK = 192
N_GX = 8
N_GY = 4
DEVICES = 32


def layout(base):
    seeded = jax.random.fold_in(base, 7)
    first, second, third = jax.random.split(seeded, 3)
    owner_perm = jax.vmap(lambda keyone: jax.random.permutation(keyone, KEY_DEV))(jax.random.split(first, DEVICES))
    device = jnp.arange(DEVICES, dtype=jnp.int32)
    along_x = device // N_GY
    along_y = device % N_GY
    owners = owner_perm // KPP
    within = owner_perm % KPP
    shuffle = jax.vmap(lambda keyone: jax.random.permutation(keyone, KEY_DEV))(jax.random.split(second, N_GX * N_GY))
    shuffle = shuffle.reshape(N_GX, N_GY, KEY_DEV)
    position = shuffle[owners, along_y[:, None], along_x[:, None] * KPP + within]
    key_slot = ((owners * N_GY + along_y[:, None]) * KEY_DEV + position).reshape(KEYS).astype(jnp.int32)
    picked = jax.vmap(lambda keyone: jax.random.permutation(keyone, KEY_DEV)[:HPD])(jax.random.split(third, DEVICES))
    heavy_keys = (device[:, None] * KEY_DEV + picked).reshape(HEAVY).astype(jnp.int32)
    slot_to_key = jnp.argsort(key_slot).astype(jnp.int32)
    heavy_flag = jnp.zeros((KEYS,), jnp.int32).at[heavy_keys].set(1)
    heavy_slot = heavy_flag[slot_to_key]
    return (key_slot, heavy_keys, slot_to_key, heavy_slot)


def draw_key_slot(key, part):
    return layout(key)[0]


def draw_heavy_keys(key, part):
    return layout(key)[1]


def draw_row_keys(key, part):
    key_slot, heavy_keys, slot_to_key, heavy_slot = layout(key)
    seeded = jax.random.fold_in(key, 11)
    favored_pool = jax.random.permutation(jax.random.fold_in(seeded, 3), N_GX)[:max(1, N_GX // 16)]
    tickets = N_GX * CAP
    pool_rank = jnp.where(heavy_slot.reshape(N_GX, OWN_SLOTS) == 1, OWN_SLOTS, 0)

    def one_device(keyone):
        parts = jax.random.split(keyone, 7)
        heavy_count = jax.random.randint(parts[0], (), ROWS_DEV // 4, ROWS_DEV // 2 + 1)
        light_count = ROWS_DEV - heavy_count
        favored = favored_pool[jax.random.randint(parts[1], (), 0, favored_pool.shape[0])]
        ticket_owner = jnp.arange(tickets, dtype=jnp.int32) // CAP
        scores = jnp.where(ticket_owner == favored, 0, tickets) + jax.random.permutation(parts[2], tickets)
        ticket_order = jnp.argsort(scores).astype(jnp.int32)
        row_index = jnp.arange(ROWS_DEV, dtype=jnp.int32)
        chosen = ticket_order[jnp.minimum(row_index, tickets - 1)]
        row_owner = chosen // CAP
        row_ticket = chosen % CAP
        mixing = jax.vmap(lambda keytwo: jax.random.permutation(keytwo, OWN_SLOTS))(jax.random.split(parts[3], N_GX))
        pools = jnp.argsort(pool_rank + mixing, axis=1)[:, :CAPK].astype(jnp.int32)
        spare = jax.random.randint(parts[4], (ROWS_DEV,), 0, CAPK)
        pool_index = jnp.where(row_ticket < CAPK, row_ticket, spare)
        light_keys = slot_to_key[row_owner * OWN_SLOTS + pools[row_owner, pool_index]]
        heavy_pick = heavy_keys[jax.random.randint(parts[5], (ROWS_DEV,), 0, HEAVY)]
        chosen_keys = jnp.where(row_index < light_count, light_keys, heavy_pick)
        return chosen_keys[jax.random.permutation(parts[6], ROWS_DEV)]
    return jax.vmap(one_device)(jax.random.split(seeded, DEVICES)).reshape(ROWS).astype(jnp.int32)


def level_of(own_key, dims, cuts, least, largest):
    factor_of = 1.0
    for dim, shards_of in cuts:
        draws = jax.random.uniform(jax.random.fold_in(jax.random.fold_in(own_key, 6), dim), (shards_of,), jnp.float32, least / len(cuts), largest / len(cuts))
        factor_of = factor_of * jnp.repeat(jnp.exp(draws), dims[dim] // shards_of).reshape((-1,) + (1,) * (len(dims) - 1 - dim))
    return factor_of


def scatter_about(rng, dims, spread, reach, pieces=(), kind=jnp.bfloat16):
    gain = level_of(rng, dims, pieces, -0.22, 0.18) if pieces else 1.0
    drawn = jax.random.normal(rng, dims, jnp.float32) * spread * gain
    return jnp.minimum(jnp.maximum(drawn, -reach), reach).astype(kind)


def setup_inputs(seed: int = 0) -> dict:
    key_list = jax.random.split(jax.random.key(seed), 6)
    return {
        "measures": scatter_about(key_list[0], (ROWS, W), 1.0, 6.0, ((0, 32),)),
        "row_keys": draw_row_keys(jax.random.fold_in(key_list[5], 71), 0),
        "orders": scatter_about(key_list[2], (KEYS, W), 1.0, 6.0, ((0, 32),)),
        "heavy_keys": draw_heavy_keys(jax.random.fold_in(key_list[5], 71), 0),
        "key_slot": draw_key_slot(jax.random.fold_in(key_list[5], 71), 0),
    }


def reference(measures, row_keys, orders, heavy_keys, key_slot):
    blocks = measures.reshape(DEVICES, ROWS_DEV, W)
    block_keys = row_keys.reshape(DEVICES, ROWS_DEV)

    def add_block(running, block_piece):
        block_rows, keys_here = block_piece
        totals = running[0] + jax.ops.segment_sum(block_rows.astype(jnp.float32), keys_here, num_segments=KEYS)
        tallies = running[1] + jax.ops.segment_sum(jnp.ones((ROWS_DEV,), jnp.float32), keys_here, num_segments=KEYS)
        return ((totals, tallies), None)
    start_state = (jnp.zeros((KEYS, W), jnp.float32), jnp.zeros((KEYS,), jnp.float32))
    (sums, counts), unused = lax.scan(add_block, start_state, (blocks, block_keys))
    joined = orders.astype(jnp.float32) * sums * lax.rsqrt(1.0 + counts)[:, None]
    result = joined.astype(jnp.bfloat16)
    heavy_report = joined[heavy_keys].astype(jnp.bfloat16)
    heavy_flag = jnp.zeros((KEYS,), jnp.float32).at[heavy_keys].set(1.0)
    slot_rows = jnp.zeros((KEYS,), jnp.float32).at[key_slot].set(counts * (1.0 - heavy_flag))
    return (result, heavy_report, slot_rows)
```

```python
import functools

import jax
import jax.numpy as jnp
from jax import lax
from jax.experimental import pallas as pl
from jax.experimental.pallas import tpu as pltpu
from jax.sharding import PartitionSpec as P

MESH = pl.DeviceIdType.MESH
LANES = 128
F32 = jnp.float32
BF16 = jnp.bfloat16
VMEM = pl.BlockSpec(memory_space=pltpu.VMEM)
ANY = pl.BlockSpec(memory_space=pl.ANY)
SMEM = pl.BlockSpec(memory_space=pltpu.SMEM)
LIMIT = 60 * 1024 * 1024
NN = (((1,), (0,)), ((), ()))
NT = (((1,), (1,)), ((), ()))


def dot(a, b, dims=NN):
    return lax.dot_general(a, b, dims, preferred_element_type=F32)


def iota(shape, dim):
    return lax.broadcasted_iota(jnp.int32, shape, dim)


def onehot(mask):
    return jnp.where(mask, 1.0, 0.0).astype(BF16)


def group_rank(flags, group_rows):
    rows = flags.shape[0]
    lane_r, lane_c = iota((LANES, LANES), 0), iota((LANES, LANES), 1)
    inside = dot(flags, onehot(lane_r < lane_c))
    whole = dot(flags, onehot(lane_r >= 0))
    row_r, row_c = iota((rows, rows), 0), iota((rows, rows), 1)
    earlier = onehot((row_c < row_r) & (row_r // group_rows == row_c // group_rows))
    return inside + dot(earlier, whole.astype(BF16))


def split(values):
    high = values.astype(BF16)
    low = (values - high.astype(F32)).astype(BF16)
    return jnp.concatenate([high, low], axis=1)


def eye(rows):
    return iota((rows, LANES), 0) == iota((rows, LANES), 1)


def encode(values):
    largest = jnp.max(jnp.abs(values), axis=1, keepdims=True)
    safe = jnp.maximum(largest, 1e-30)
    fixed = jnp.round(values * (1.0 / safe) * 32767.0).astype(jnp.int32).astype(jnp.int16)
    return fixed, jnp.sum(jnp.where(eye(values.shape[0]), safe, 0.0), axis=0, keepdims=True)


def decode(fixed, scale):
    column = jnp.sum(jnp.where(eye(fixed.shape[0]), scale, 0.0), axis=1, keepdims=True)
    return fixed.astype(jnp.int32).astype(F32) * (column * (1.0 / 32767.0))


def pieces(total):
    return [(at, min(LANES, total - at)) for at in range(0, total, LANES)]


def byte_table(table, parts):
    pieces = [((table >> (8 * p)) & 255).astype(F32).T for p in range(parts)]
    return jnp.concatenate(pieces, axis=0).astype(BF16)


def look_up(bytes_table, row_hot, column_mask, parts):
    wide = dot(bytes_table, row_hot)
    found = 0.0
    for p in range(parts):
        piece = wide[p * LANES : (p + 1) * LANES]
        found = found + float(256**p) * jnp.sum(
            jnp.where(column_mask, piece, 0.0), axis=0, keepdims=True
        )
    return found.astype(jnp.int32)


def byte_count(largest):
    return (int(largest).bit_length() + 7) // 8


def gather_rows(cfg, measures, keys, heavy, key_slot, send, tally, small, slots, sums):
    rows, block, nr = cfg["rows"], cfg["block"], cfg["nr"]
    segments, capacity = cfg["segments"], cfg["capacity"]
    slot_parts = byte_count(nr * LANES - 1)
    slot_bytes = byte_table(key_slot[...], slot_parts)
    hist_key = jnp.zeros((nr, LANES), F32)
    hist_slot = jnp.zeros((nr, LANES), F32)
    heavy_sum = jnp.zeros((cfg["heavy"], LANES), F32)
    for c in range(rows // block):
        span = slice(c * block, (c + 1) * block)
        key = keys[:, span]
        row_hot = onehot(iota((nr, block), 0) == key >> 7)
        column_mask = iota((LANES, block), 0) == (key & 127)
        hist_key = hist_key + dot(row_hot, onehot(column_mask), NT)
        heavy_hot = jnp.where(heavy[...] == key, 1.0, 0.0)
        is_heavy = jnp.max(heavy_hot, axis=0, keepdims=True) > 0.0
        heavy_sum = heavy_sum + dot(heavy_hot.astype(BF16), measures[span, :])
        slot = jnp.where(is_heavy, -1, look_up(slot_bytes, row_hot, column_mask, slot_parts))
        slots[:, span] = slot
        slot_row = onehot(iota((nr, block), 0) == slot >> 7)
        slot_column = onehot(iota((LANES, block), 0) == (slot & 127))
        hist_slot = hist_slot + dot(slot_row, slot_column, NT)
    present = hist_slot > 0.0
    group = cfg["own"] // LANES
    tally[...] = jnp.zeros(tally.shape, F32)
    for x in range(cfg["gx"]):
        tally[x, 0:group, :] = hist_slot[x * group : (x + 1) * group]
    rank = group_rank(onehot(present), group).astype(jnp.int32)
    owner = iota((nr, LANES), 0) // group
    segment_table = jnp.where(present, owner * capacity + rank + 1, 0)
    seg_parts = byte_count(segments)
    segment_bytes = byte_table(segment_table, seg_parts)
    step = cfg["seg_block"]
    for c in range(rows // block):
        span = slice(c * block, (c + 1) * block)
        slot = slots[:, span]
        slot_row = onehot(iota((nr, block), 0) == slot >> 7)
        slot_mask = iota((LANES, block), 0) == (slot & 127)
        segment = look_up(segment_bytes, slot_row, slot_mask, seg_parts) - 1
        for s in range(segments // step):
            hot = onehot(iota((step, block), 0) == segment - s * step)
            product = dot(hot, measures[span, :])
            place = slice(s * step, (s + 1) * step)
            if c == 0:
                sums[place, :] = product
            else:
                sums[place, :] += product
    for x in range(cfg["gx"]):
        for p, (at, size) in enumerate(pieces(capacity)):
            first = x * capacity + at
            fixed, scale = encode(sums[first : first + size, :])
            send[x, at : at + size, :] = fixed
            tally[x, group + p : group + p + 1, :] = scale
    each, key_rows, height = cfg["heavy_each"], cfg["key_rows"], cfg["height"]
    small[...] = jnp.zeros(small.shape, F32)
    for d in range(cfg["devices"]):
        small[d * height : d * height + each, :] = heavy_sum[d * each : (d + 1) * each]
        top = (d + 1) * height
        small[top - key_rows : top, :] = hist_key[d * key_rows : (d + 1) * key_rows]


def place_rows(cfg, got, got_tally, key_slot, send, scales, tally, spread, ranks):
    gx, gy, own, kpp = cfg["gx"], cfg["gy"], cfg["own"], cfg["kpp"]
    key_rows, capacity = cfg["key_rows"], cfg["capacity"]
    group = own // LANES
    base = lax.axis_index("gx") * own
    local = key_slot[...] - base
    mine = (local >= 0) & (local < own)
    rank = jnp.where(mine, group_rank(onehot(mine), key_rows), -1.0).astype(jnp.int32)
    local = local.astype(F32)
    for y in range(gy):
        for x in range(gx):
            first = (x * gy + y) * key_rows
            acc = jnp.zeros((kpp, LANES), F32)
            for j in range(key_rows):
                hit = iota((kpp, LANES), 0) == rank[first + j : first + j + 1]
                acc = acc + jnp.where(hit, local[first + j : first + j + 1], 0.0)
            at = (y * gx + x) * kpp
            spread[at : at + kpp, :] = acc
    counts = jnp.concatenate([got_tally[i, 0:group, :] for i in range(gx)], axis=0)
    present = counts > 0.0
    ranks[...] = jnp.where(present, group_rank(onehot(present), group) + 1.0, 0.0)
    total = counts[0:group]
    for i in range(1, gx):
        total = total + counts[i * group : (i + 1) * group]
    tally[...] = total
    values = []
    for i in range(gx):
        decoded = [
            decode(got[i, at : at + size, :], got_tally[i, group + p : group + p + 1, :])
            for p, (at, size) in enumerate(pieces(capacity))
        ]
        values.append(split(jnp.concatenate(decoded, axis=0)))
    quarter = own // gy
    for q in range(gy):
        at = slice(q * quarter, (q + 1) * quarter)
        slot = jnp.sum(spread[at, :], axis=1, keepdims=True).astype(jnp.int32) - q * quarter
        found = jnp.zeros((quarter, gx), F32)
        for j in range(key_rows):
            hot = onehot(slot - j * LANES == iota((quarter, LANES), 1))
            table = ranks[pl.ds(q * key_rows + j, gx, stride=group), :].astype(BF16)
            found = found + dot(hot, table, NT)
        found = found.astype(jnp.int32) - 1
        out = jnp.zeros((quarter, 2 * LANES), F32)
        for i in range(gx):
            hot = onehot(found[:, i : i + 1] == iota((quarter, capacity), 1))
            out = out + dot(hot, values[i])
        out = out[:, :LANES] + out[:, LANES:]
        for x in range(gx):
            fixed, scale = encode(out[x * kpp : (x + 1) * kpp])
            send[q * gx + x] = fixed
            scales[q * gx + x] = scale


def join_rows(cfg, heavy, got, got_scales, got_small, got_tally, orders, key_slot, result, report, slot_rows, sums, joined):
    gx, gy, own, kpp = cfg["gx"], cfg["gy"], cfg["own"], cfg["kpp"]
    key_rows, height, each = cfg["key_rows"], cfg["height"], cfg["heavy_each"]
    key_dev = key_rows * LANES
    device = lax.axis_index("gx") * gy + lax.axis_index("gy")
    total = got_tally[0:key_rows]
    for y in range(1, gy):
        total = total + got_tally[y * key_rows : (y + 1) * key_rows]
    slot_rows[...] = total
    small = got_small[0:height]
    for d in range(1, cfg["devices"]):
        small = small + got_small[d * height : (d + 1) * height]
    for x in range(gx):
        part = decode(got[x * gy], got_scales[x * gy])
        for y in range(1, gy):
            part = part + decode(got[x * gy + y], got_scales[x * gy + y])
        sums[x * kpp : (x + 1) * kpp, :] = part
    values = split(sums[...])
    owner = key_slot[pl.ds(device * key_rows, key_rows), :] // own
    flags = jnp.concatenate([jnp.where(owner == x, 1.0, 0.0) for x in range(gx)], axis=0)
    rank = group_rank(flags.astype(BF16), key_rows)
    place = jnp.zeros((key_rows, LANES), F32)
    for x in range(gx):
        here = rank[x * key_rows : (x + 1) * key_rows] + float(x * kpp)
        place = place + jnp.where(owner == x, here, 0.0)
    counts = small[height - key_rows : height]
    stacked = jnp.concatenate([place, counts], axis=0)
    columns = stacked.T
    for j in range(key_rows):
        at = slice(j * LANES, (j + 1) * LANES)
        where = columns[:, j : j + 1].astype(jnp.int32)
        hot = onehot(where == iota((LANES, key_dev), 1))
        both = dot(hot, values)
        found = both[:, :LANES] + both[:, LANES:]
        for h in range(each):
            spot = heavy[device * each + h] - device * key_dev - j * LANES
            found = found + jnp.where(iota((LANES, LANES), 0) == spot, small[h : h + 1], 0.0)
        scale = lax.rsqrt(1.0 + columns[:, key_rows + j : key_rows + j + 1])
        value = orders[at, :].astype(F32) * found * scale
        joined[at, :] = value
        result[at, :] = value.astype(BF16)
    lines = [
        joined[pl.ds(heavy[device * each + h] - device * key_dev, 1), :] for h in range(each)
    ]
    report[...] = jnp.concatenate(lines, axis=0).astype(BF16)


def all_barrier(gx, gy, me_x, me_y):
    barrier = pltpu.get_barrier_semaphore()
    device = me_x * gy + me_y
    devices = gx * gy

    @pl.loop(1, devices)
    def _(step):
        other = lax.rem(device + step, devices)
        target = (other // gy, lax.rem(other, gy))
        pl.semaphore_signal(barrier, inc=1, device_id=target, device_id_type=MESH)

    pl.semaphore_wait(barrier, devices - 1)


def exchange(me, count, moves, address):
    for source, landing, send_sem, recv_sem, local_sem in moves:
        pltpu.make_async_copy(source(me), landing(me), local_sem).start()

    def remote(other, move):
        source, landing, send_sem, recv_sem, local_sem = move
        return pltpu.make_async_remote_copy(
            src_ref=source(other),
            dst_ref=landing(me),
            send_sem=send_sem.at[other],
            recv_sem=recv_sem.at[me],
            device_id=address(other),
            device_id_type=MESH,
        )

    def finish(other, move):
        source, landing, send_sem, recv_sem, local_sem = move
        copy = pltpu.make_async_remote_copy(
            src_ref=source(other),
            dst_ref=landing(other),
            send_sem=send_sem.at[other],
            recv_sem=recv_sem.at[other],
            device_id=address(other),
            device_id_type=MESH,
        )
        copy.wait_send()
        copy.wait_recv()

    @pl.loop(1, count)
    def _(step):
        for move in moves:
            remote(lax.rem(me + step, count), move).start()

    def end():
        @pl.loop(1, count)
        def _(step):
            for move in moves:
                finish(lax.rem(me + step, count), move)

        for source, landing, send_sem, recv_sem, local_sem in moves:
            pltpu.make_async_copy(source(me), landing(me), local_sem).wait()

    return end


def to_owners(gx, gy, send, tally, small, got, got_tally, got_small, sem_a, sem_b, sem_c, sem_d, sem_e, sem_f, local):
    me_x, me_y = lax.axis_index("gx"), lax.axis_index("gy")
    all_barrier(gx, gy, me_x, me_y)
    rows = (lambda i: send.at[i], lambda i: got.at[i], sem_a, sem_b, local.at[0])
    tallies = (lambda i: tally.at[i], lambda i: got_tally.at[i], sem_c, sem_d, local.at[1])
    end_x = exchange(me_x, gx, [rows, tallies], lambda i: (i, me_y))
    others = (lambda i: small.at[i], lambda i: got_small.at[i], sem_e, sem_f, local.at[2])
    end_all = exchange(
        me_x * gy + me_y, gx * gy, [others], lambda i: (i // gy, lax.rem(i, gy))
    )
    end_x()
    end_all()


def to_ranges(gx, gy, send, scales, tally, got, got_scales, got_tally, sem_a, sem_b, sem_c, sem_d, sem_e, sem_f, local):
    me_x, me_y = lax.axis_index("gx"), lax.axis_index("gy")
    all_barrier(gx, gy, me_x, me_y)
    rows = (
        lambda i: send.at[lax.rem(i, gy) * gx + i // gy],
        lambda i: got.at[i],
        sem_a,
        sem_b,
        local.at[0],
    )
    factors = (
        lambda i: scales.at[lax.rem(i, gy) * gx + i // gy],
        lambda i: got_scales.at[i],
        sem_e,
        sem_f,
        local.at[2],
    )
    end_all = exchange(
        me_x * gy + me_y, gx * gy, [rows, factors], lambda i: (i // gy, lax.rem(i, gy))
    )
    tallies = (lambda i: tally.at[i], lambda i: got_tally.at[i], sem_c, sem_d, local.at[1])
    end_y = exchange(me_y, gy, [tallies], lambda i: (me_x, i))
    end_y()
    end_all()


def shaped(*dims, dtype=F32):
    return jax.ShapeDtypeStruct(dims, dtype)


def split_body(measures, row_keys, orders, heavy_keys, key_slot):
    rows, columns = measures.shape
    gx, gy = lax.axis_size("gx"), lax.axis_size("gy")
    devices = gx * gy
    key_dev = orders.shape[0]
    key_rows = key_dev // LANES
    own = key_dev * gy
    nr = key_slot.shape[0] // LANES
    heavy = heavy_keys.shape[0]
    each = heavy // devices
    capacity = max(rows // 32, 3 * rows // (4 * gx)) // 4
    segments = gx * capacity
    cfg = dict(
        rows=rows,
        block=min(rows, 2048),
        nr=nr,
        gx=gx,
        gy=gy,
        devices=devices,
        own=own,
        kpp=key_dev // gx,
        key_rows=key_rows,
        heavy=heavy,
        heavy_each=each,
        height=-(-(each + key_rows) // 8) * 8,
        capacity=capacity,
        segments=segments,
        seg_block=512 if segments % 512 == 0 else segments,
    )
    height = cfg["height"]
    group = own // LANES
    params = pltpu.CompilerParams(vmem_limit_bytes=LIMIT)
    table = key_slot.reshape(nr, LANES)
    kpp = cfg["kpp"]
    tall = group + -(-len(pieces(capacity)) // 8) * 8
    send, tally, small = pl.pallas_call(
        functools.partial(gather_rows, cfg),
        out_shape=(
            shaped(gx, capacity, columns, dtype=jnp.int16),
            shaped(gx, tall, LANES),
            shaped(devices * height, LANES),
        ),
        in_specs=[VMEM] * 4,
        out_specs=(VMEM,) * 3,
        scratch_shapes=[pltpu.VMEM((1, rows), jnp.int32), pltpu.VMEM((segments, columns), F32)],
        compiler_params=params,
    )(measures, row_keys.reshape(1, rows), heavy_keys.reshape(heavy, 1), table)
    dma = pltpu.SemaphoreType.DMA
    got, got_tally, got_small = pl.pallas_call(
        functools.partial(to_owners, gx, gy),
        out_shape=(
            shaped(gx, capacity, columns, dtype=jnp.int16),
            shaped(gx, tall, LANES),
            shaped(devices, height, LANES),
        ),
        in_specs=[ANY] * 3,
        out_specs=(ANY,) * 3,
        scratch_shapes=[dma((gx,))] * 4 + [dma((devices,))] * 2 + [dma((3,))],
        compiler_params=pltpu.CompilerParams(collective_id=0, has_side_effects=True),
    )(send, tally, small.reshape(devices, height, LANES))
    send2, scales2, tally2 = pl.pallas_call(
        functools.partial(place_rows, cfg),
        out_shape=(
            shaped(devices, kpp, columns, dtype=jnp.int16),
            shaped(devices, 1, LANES),
            shaped(group, LANES),
        ),
        in_specs=[VMEM] * 3,
        out_specs=(VMEM,) * 3,
        scratch_shapes=[pltpu.VMEM((own, LANES), F32), pltpu.VMEM((gx * group, LANES), F32)],
        compiler_params=params,
    )(got, got_tally, table)
    got2, got_scales2, got_tally2 = pl.pallas_call(
        functools.partial(to_ranges, gx, gy),
        out_shape=(
            shaped(devices, kpp, columns, dtype=jnp.int16),
            shaped(devices, 1, LANES),
            shaped(gy, key_rows, LANES),
        ),
        in_specs=[ANY] * 3,
        out_specs=(ANY,) * 3,
        scratch_shapes=[dma((devices,))] * 2
        + [dma((gy,))] * 2
        + [dma((devices,))] * 2
        + [dma((3,))],
        compiler_params=pltpu.CompilerParams(collective_id=1, has_side_effects=True),
    )(send2, scales2, tally2.reshape(gy, key_rows, LANES))
    result, report, slot_rows = pl.pallas_call(
        functools.partial(join_rows, cfg),
        out_shape=(
            shaped(key_dev, columns, dtype=BF16),
            shaped(each, columns, dtype=BF16),
            shaped(key_rows, LANES),
        ),
        in_specs=[SMEM] + [VMEM] * 6,
        out_specs=(VMEM,) * 3,
        scratch_shapes=[pltpu.VMEM((key_dev, LANES), F32)] * 2,
        compiler_params=params,
    )(
        heavy_keys,
        got2,
        got_scales2,
        got_small.reshape(devices * height, LANES),
        got_tally2.reshape(gy * key_rows, LANES),
        orders,
        table,
    )
    return (result, report, slot_rows.reshape(key_dev))


def fused(
    cfg, measures, keys, heavy, table,
    got2, scales2, hgot, total_out, slot_out,
    rows_in, seg_hot, group_row, local_row, hist, hist16, send1, got1, goth, cnt_got,
    codes, ranks, found, wide, hsend, send2, srow, tsend, tgot,
    load_sem, cs, cr, hs, hr, rs, rr, ys, yr, ss, sr, zs, zr, ts, tr, own_sem,
):
    gx, gy, nr, rows, block = cfg["gx"], cfg["gy"], cfg["nr"], cfg["rows"], cfg["block"]
    devices, own, kpp, key_rows = cfg["devices"], cfg["own"], cfg["kpp"], cfg["key_rows"]
    cap, extra, seg, deep = cfg["cap"], cfg["extra"], cfg["seg"], cfg["deep"]
    each, planes = cfg["each"], cfg["planes"]
    key_dev = key_rows * LANES
    per_tile = LANES // kpp
    mx, my = lax.axis_index("gx"), lax.axis_index("gy")
    me = mx * gy + my
    z, j = me // gx, lax.rem(me, gx)

    def mesh_id(d):
        return (d // gy, lax.rem(d, gy))

    def remote(src, dst, send_sem, recv_sem, d):
        return pltpu.make_async_remote_copy(
            src_ref=src, dst_ref=dst, send_sem=send_sem, recv_sem=recv_sem,
            device_id=mesh_id(d), device_id_type=MESH,
        )

    barrier = pltpu.get_barrier_semaphore()

    @pl.loop(1, devices)
    def _(step):
        pl.semaphore_signal(
            barrier, inc=1, device_id=mesh_id(lax.rem(me + step, devices)), device_id_type=MESH
        )

    load = pltpu.make_async_copy(measures, rows_in, load_sem)
    load.start()

    total = jnp.zeros((nr, LANES), F32)
    for c in range(rows // block):
        span = slice(c * block, (c + 1) * block)
        key = keys[:, span]
        row_hot = onehot(iota((nr, block), 0) == key >> 7)
        seg_hot[:, span] = row_hot
        total = total + dot(row_hot, onehot(iota((LANES, block), 0) == (key & 127)), NT)
    hist[...] = total.reshape(devices, key_rows, LANES)
    hist16[...] = total.astype(jnp.int32).astype(jnp.int16)
    cnt_got[me] = hist[me]

    pl.semaphore_wait(barrier, devices - 1)

    @pl.loop(0, gx - 1)
    def _(s):
        x = lax.rem(j + 1 + s, gx)
        t = lax.rem(2 * gx - 2 - s, gx)
        remote(hist16, goth.at[t], hs.at[s], hr.at[t], z * gx + x).start()

    @pl.loop(1, devices)
    def _(s):
        d = lax.rem(me + s, devices)
        remote(hist.at[d], cnt_got.at[me], cs.at[d], cr.at[me], d).start()

    owner = table[...] // own
    heavy_key = heavy[...]
    heads = heavy_key.shape[1]
    code = iota((1, heads), 1) + 1
    row_of = iota((nr, heads), 0) == heavy_key >> 7
    col_of = onehot(iota((LANES, heads), 0) == (heavy_key & 127))
    low = dot(jnp.where(row_of, (code & 127).astype(F32), 0.0).astype(BF16), col_of, NT)
    high = dot(jnp.where(row_of, (code >> 7).astype(F32), 0.0).astype(BF16), col_of, NT)
    which = (low + 128.0 * high).astype(jnp.int32)
    codes[...] = which.astype(F32).reshape(devices, key_rows, LANES)
    light = which == 0
    present = (total > 0.0) & light
    lane_r, lane_c = iota((LANES, 2 * LANES), 0), iota((LANES, 2 * LANES), 1)
    upper = onehot((lane_c >= LANES) | (lane_r < lane_c))
    lower = onehot(iota((nr, nr), 1) < iota((nr, nr), 0))
    flags = jnp.concatenate(
        [jnp.where(present & (owner == x), 1.0, 0.0) for x in range(gx)], axis=0
    ).astype(BF16)
    both = dot(flags, upper)
    local = jnp.zeros((nr, LANES), F32)
    for x in range(gx):
        part = both[x * nr : (x + 1) * nr]
        rank = part[:, :LANES] + dot(lower, part[:, LANES:].astype(BF16))
        local = local + jnp.where(owner == x, rank, 0.0)
    head = which - 1
    block_of = head // each
    group = jnp.where(light, owner, lax.rem(block_of, gx))
    local = jnp.where(
        light, local, (cap + (block_of // gx) * each + lax.rem(head, each)).astype(F32)
    )
    tables = jnp.concatenate([group.astype(F32).T, local.T], axis=0).astype(BF16)
    for c in range(rows // block):
        span = slice(c * block, (c + 1) * block)
        spread = dot(tables, seg_hot[:, span])
        mask = iota((LANES, block), 0) == (keys[:, span] & 127)
        group_row[:, span] = jnp.sum(
            jnp.where(mask, spread[:LANES], 0.0), axis=0, keepdims=True
        ).astype(jnp.int32)
        local_row[:, span] = jnp.sum(
            jnp.where(mask, spread[LANES:], 0.0), axis=0, keepdims=True
        ).astype(jnp.int32)

    load.wait()
    shifts = seg - cap - extra

    def encode(values):
        largest = jnp.max(jnp.abs(values), axis=1, keepdims=True)
        power = jnp.floor(jnp.log2(jnp.maximum(largest, 1e-30))) + 1.0
        fixed = jnp.clip(jnp.round(values * jnp.exp2(15.0 - power)), -32767.0, 32767.0)
        return fixed, power

    @pl.loop(0, gx)
    def _(s):
        x = lax.rem(j + 1 + s, gx)
        acc = jnp.zeros((seg, LANES), F32)
        for c in range(rows // block):
            span = slice(c * block, (c + 1) * block)
            place = jnp.where(group_row[:, span] == x, local_row[:, span], -1)
            acc = acc + dot(onehot(iota((seg, block), 0) == place), rows_in[span, :])
        fixed, power = encode(acc)
        lines = []
        for at, size in pieces(cap + extra):
            diagonal = iota((size, LANES), 0) == iota((size, LANES), 1)
            lines.append(
                jnp.sum(jnp.where(diagonal, power[at : at + size], 0.0), axis=0, keepdims=True)
            )
        lines.append(jnp.zeros((shifts - len(lines), LANES), F32))
        whole = jnp.concatenate([fixed[: cap + extra]] + lines, axis=0)
        send1[s] = whole.astype(jnp.int32).astype(jnp.int16)

        @pl.when(s < gx - 1)
        def _():
            t = lax.rem(2 * gx - 2 - s, gx)
            remote(send1.at[s], got1.at[t], rs.at[s], rr.at[t], z * gx + x).start()

    for t in range(gx - 1):
        remote(hist16, goth.at[t], hs.at[gx - 2 - t], hr.at[t], me).wait_recv()
    mine = (owner == j) & light
    arrived = []
    for t in range(gx):
        here = hist16[...] if t == gx - 1 else goth[t]
        arrived.append(jnp.where((here.astype(jnp.int32) > 0) & mine, 1.0, 0.0))
    flags = jnp.concatenate(arrived, axis=0)
    both = dot(flags.astype(BF16), upper)
    for t in range(gx):
        part = both[t * nr : (t + 1) * nr]
        rank = part[:, :LANES] + dot(lower, part[:, LANES:].astype(BF16)) + 1.0
        ranks[t * nr : (t + 1) * nr, :] = rank * flags[t * nr : (t + 1) * nr]
    own_flags = onehot(owner == j)
    both = dot(own_flags, upper)
    row_r, row_c = iota((nr, nr), 0), iota((nr, nr), 1)
    near = onehot((row_c < row_r) & (row_r // key_rows == row_c // key_rows))
    rank = both[:, :LANES] + dot(near, both[:, LANES:].astype(BF16))
    rank = jnp.where(owner == j, rank, -1.0).astype(jnp.int32)
    for d in range(devices):
        hot, tall = [], []
        for q in range(key_rows):
            r = d * key_rows + q
            hot.append(onehot(iota((kpp, LANES), 0) == rank[r : r + 1]))
            tall.append(ranks[pl.ds(r, gx, stride=nr), :].astype(BF16))
        found[d * kpp : (d + 1) * kpp, 0:gx] = dot(
            jnp.concatenate(hot, axis=1), jnp.concatenate(tall, axis=1), NT
        )

    @pl.loop(1, devices)
    def _(s):
        d = lax.rem(me + s, devices)
        remote(hist.at[d], cnt_got.at[d], cs.at[d], cr.at[d], d).wait()

    counted = cnt_got[0]
    for d in range(1, devices):
        counted = counted + cnt_got[d]
    total_out[...] = counted
    tsend[...] = jnp.where(codes[me] == 0.0, counted, 0.0)
    tgot[mx] = tsend[...]

    @pl.loop(1, gx)
    def _(s):
        x = lax.rem(mx + s, gx)
        remote(tsend, tgot.at[mx], ts.at[x], tr.at[mx], x * gy + my).start()

    heads_sum = jnp.zeros((extra, LANES), F32)
    powers = []
    for t in range(gx):
        if t < gx - 1:
            remote(send1.at[t], got1.at[t], rs.at[gx - 2 - t], rr.at[t], me).wait_recv()
            block16 = got1[t]
        else:
            block16 = send1[t]
        value = block16.astype(jnp.int32)
        wide[t, 0:seg, :LANES] = (value >> 8).astype(F32).astype(BF16)
        wide[t, 0:seg, LANES:] = (value & 255).astype(F32).astype(BF16)
        if deep > seg:
            wide[t, seg:deep, :] = jnp.zeros((deep - seg, 2 * LANES), BF16)
        scale = jnp.exp2(value[cap + extra :].astype(F32) - 15.0)
        line = jnp.concatenate(
            [scale[p : p + 1] for p in range(deep // LANES)], axis=1
        )
        powers.append(line)
        p, at = cap // LANES, cap % LANES
        column = jnp.sum(
            jnp.where(iota((extra, LANES), 1) == iota((extra, LANES), 0) + at, scale[p : p + 1], 0.0),
            axis=1, keepdims=True,
        )
        heads_sum = heads_sum + value[cap : cap + extra].astype(F32) * column
    hsend[...] = heads_sum

    local_heads = pltpu.make_async_copy(hsend, hgot.at[z], own_sem.at[0])
    local_heads.start()

    @pl.loop(1, planes)
    def _(s):
        other = lax.rem(z + s, planes)
        remote(hsend, hgot.at[z], zs.at[other], zr.at[z], other * gx + j).start()

    chunk = gx * kpp
    shift = lax.rem(j, per_tile) * kpp
    half = planes // 2
    if planes == 4:
        order = [
            lax.rem(z + half, planes), planes - 1 - z,
            planes - 1 - lax.rem(z + half, planes), z,
        ]
    else:
        order = [lax.rem(z + s, planes) for s in range(1, planes + 1)]
    for c in range(planes):
        far = order[c]
        spot = found[pl.ds(pl.multiple_of(far * chunk, chunk), chunk), :]
        acc = jnp.zeros((chunk, 2 * LANES), F32)
        for t in range(gx):
            hit = spot[:, t : t + 1].astype(jnp.int32) == iota((chunk, deep), 1) + 1
            acc = acc + dot(jnp.where(hit, powers[t], 0.0).astype(BF16), wide[t])
        fixed, power = encode(acc[:, :LANES] * 256.0 + acc[:, LANES:])
        send2[c] = fixed.astype(jnp.int32).astype(jnp.int16).reshape(gx, kpp, LANES)
        scale = jnp.exp2(power - 15.0)
        diagonal = iota((kpp, LANES), 1) == iota((kpp, LANES), 0) + shift
        for x in range(gx):
            srow[c, x] = jnp.sum(
                jnp.where(diagonal, scale[x * kpp : (x + 1) * kpp], 0.0), axis=0, keepdims=True
            )
        last = c == planes - 1

        @pl.loop(0, gx - 1 if last else gx)
        def _(s):
            x = lax.rem(j + 1 + s, gx)
            d = far * gx + x
            remote(send2.at[c, x], got2.at[me], ys.at[d], yr.at[me], d).start()
            remote(srow.at[c, x], scales2.at[me], ss.at[d], sr.at[me], d).start()

        if last:
            keep = pltpu.make_async_copy(send2.at[c, j], got2.at[me], own_sem.at[1])
            keep.start()
            keep_row = pltpu.make_async_copy(srow.at[c, j], scales2.at[me], own_sem.at[2])
            keep_row.start()

    @pl.loop(1, gx)
    def _(s):
        x = lax.rem(mx + s, gx)
        remote(tsend, tgot.at[x], ts.at[x], tr.at[x], x * gy + my).wait()

    base = me * key_dev
    left, right = [], []
    for m in range(gx):
        slots = table[pl.ds((m * gy + my) * key_rows, key_rows), :] - base
        for q in range(key_rows):
            line = slots[q : q + 1]
            amount = tgot[m, q : q + 1, :].astype(jnp.int32)
            bands = [
                jnp.where(
                    iota((8, LANES), 0) == (line >> 7), ((amount >> (8 * b)) & 255).astype(F32), 0.0
                )
                for b in range(3)
            ]
            left.append(jnp.concatenate(bands + [jnp.zeros((8, LANES), F32)], axis=0).astype(BF16))
            right.append(onehot(iota((LANES, LANES), 0) == (line & 127)))
    bands = dot(jnp.concatenate(left, axis=1), jnp.concatenate(right, axis=1), NT)
    slot_out[...] = (bands[0:8] + 256.0 * bands[8:16] + 65536.0 * bands[16:24])[0:key_rows]

    for s in range(gx - 1):
        t = (2 * gx - 2 - s) % gx
        remote(hist16, goth.at[t], hs.at[s], hr.at[t], me).wait_send()
        remote(send1.at[s], got1.at[t], rs.at[s], rr.at[t], me).wait_send()
    local_heads.wait()
    keep.wait()
    keep_row.wait()

    @pl.loop(1, planes)
    def _(s):
        other = lax.rem(z + s, planes)
        remote(hsend, hgot.at[other], zs.at[other], zr.at[other], other * gx + j).wait()

    @pl.loop(1, devices)
    def _(s):
        d = lax.rem(me + s, devices)
        remote(send2.at[0, 0], got2.at[d], ys.at[d], yr.at[d], d).wait()
        remote(srow.at[0, 0], scales2.at[d], ss.at[d], sr.at[d], d).wait()


def join(cfg, heavy, got, scales, heads, total, slot_in, orders, table, result, report, slot_rows, joined):
    gx, gy, own, kpp = cfg["gx"], cfg["gy"], cfg["own"], cfg["kpp"]
    key_rows, each, planes, extra = cfg["key_rows"], cfg["each"], cfg["planes"], cfg["extra"]
    key_dev = key_rows * LANES
    per_tile = LANES // kpp
    device = lax.axis_index("gx") * gy + lax.axis_index("gy")
    slot_rows[...] = slot_in[...]
    z = device // gx
    small = heads[0]
    for p in range(1, planes):
        small = small + heads[p]
    owner = table[pl.ds(device * key_rows, key_rows), :] // own
    flags = jnp.concatenate([jnp.where(owner == x, 1.0, 0.0) for x in range(gx)], axis=0)
    rank = group_rank(flags.astype(BF16), key_rows)
    place = jnp.zeros((key_rows, LANES), F32)
    for x in range(gx):
        here = rank[x * key_rows : (x + 1) * key_rows] + float(x * kpp)
        place = place + jnp.where(owner == x, here, 0.0)
    columns = jnp.concatenate([place, total[...]], axis=0).T
    values, lines = [], []
    for p in range(planes):
        value = got[p * gx : (p + 1) * gx].reshape(key_dev, LANES).astype(jnp.int32)
        values.append(
            jnp.concatenate([(value >> 8).astype(F32), (value & 255).astype(F32)], axis=1).astype(BF16)
        )
        tiles = []
        for x in range(0, gx, per_tile):
            tile = scales[p * gx + x]
            for i in range(1, per_tile):
                tile = tile + scales[p * gx + x + i]
            tiles.append(tile)
        lines.append(jnp.concatenate(tiles, axis=1))
    for j in range(key_rows):
        at = slice(j * LANES, (j + 1) * LANES)
        hit = columns[:, j : j + 1].astype(jnp.int32) == iota((LANES, key_dev), 1)
        both = jnp.zeros((LANES, 2 * LANES), F32)
        for p in range(planes):
            both = both + dot(jnp.where(hit, lines[p], 0.0).astype(BF16), values[p])
        sums = both[:, :LANES] * 256.0 + both[:, LANES:]
        for h in range(each):
            spot = heavy[device * each + h] - device * key_dev - j * LANES
            line = jnp.sum(
                jnp.where(iota((extra, LANES), 0) == z * each + h, small, 0.0), axis=0, keepdims=True
            )
            sums = sums + jnp.where(iota((LANES, LANES), 0) == spot, line, 0.0)
        scale = lax.rsqrt(1.0 + columns[:, key_rows + j : key_rows + j + 1])
        value = orders[at, :].astype(F32) * sums * scale
        joined[at, :] = value
        result[at, :] = value.astype(BF16)
    picked = [
        joined[pl.ds(heavy[device * each + h] - device * key_dev, 1), :] for h in range(each)
    ]
    report[...] = jnp.concatenate(picked, axis=0).astype(BF16)


def body(measures, row_keys, orders, heavy_keys, key_slot):
    rows, columns = measures.shape
    gx, gy = lax.axis_size("gx"), lax.axis_size("gy")
    devices = gx * gy
    key_dev = orders.shape[0]
    key_rows = key_dev // LANES
    nr = key_slot.shape[0] // LANES
    heavy = heavy_keys.shape[0]
    each = heavy // devices
    if gx * nr > 2048:
        return split_body(measures, row_keys, orders, heavy_keys, key_slot)
    planes = devices // gx
    cap = max(rows // 32, 3 * rows // (4 * gx)) // 4
    extra = planes * each
    seg = -(-(cap + extra + len(pieces(cap + extra))) // 16) * 16
    deep = -(-cap // LANES) * LANES
    kpp = key_dev // gx
    cfg = dict(
        rows=rows, block=min(rows, 2048), nr=nr, gx=gx, gy=gy, devices=devices,
        own=key_dev * gy, kpp=kpp, key_rows=key_rows, each=each, planes=planes,
        cap=cap, extra=extra, seg=seg, deep=max(deep, -(-seg // LANES) * LANES),
    )
    deep = cfg["deep"]
    table = key_slot.reshape(nr, LANES)
    dma = pltpu.SemaphoreType.DMA
    i16 = jnp.int16
    got, scales, heads, total, slots = pl.pallas_call(
        functools.partial(fused, cfg),
        out_shape=(
            shaped(devices, kpp, columns, dtype=i16),
            shaped(devices, 1, LANES),
            shaped(planes, extra, LANES),
            shaped(key_rows, LANES),
            shaped(key_rows, LANES),
        ),
        in_specs=[ANY] + [VMEM] * 3,
        out_specs=(ANY,) * 3 + (VMEM,) * 2,
        scratch_shapes=[
            pltpu.VMEM((rows, columns), BF16),
            pltpu.VMEM((nr, rows), BF16),
            pltpu.VMEM((1, rows), jnp.int32),
            pltpu.VMEM((1, rows), jnp.int32),
            pltpu.VMEM((devices, key_rows, LANES), F32),
            pltpu.VMEM((nr, LANES), i16),
            pltpu.VMEM((gx, seg, LANES), i16),
            pltpu.VMEM((gx, seg, LANES), i16),
            pltpu.VMEM((gx, nr, LANES), i16),
            pltpu.VMEM((devices, key_rows, LANES), F32),
            pltpu.VMEM((devices, key_rows, LANES), F32),
            pltpu.VMEM((gx * nr, LANES), F32),
            pltpu.VMEM((devices * kpp, LANES), F32),
            pltpu.VMEM((gx, deep, 2 * LANES), BF16),
            pltpu.VMEM((extra, LANES), F32),
            pltpu.VMEM((planes, gx, kpp, LANES), i16),
            pltpu.VMEM((planes, gx, 1, LANES), F32),
            pltpu.VMEM((key_rows, LANES), F32),
            pltpu.VMEM((gx, key_rows, LANES), F32),
            dma,
            dma((devices,)), dma((devices,)),
            dma((gx,)), dma((gx,)),
            dma((gx,)), dma((gx,)),
            dma((devices,)), dma((devices,)),
            dma((devices,)), dma((devices,)),
            dma((planes,)), dma((planes,)),
            dma((gx,)), dma((gx,)),
            dma((3,)),
        ],
        compiler_params=pltpu.CompilerParams(
            collective_id=2, has_side_effects=True, vmem_limit_bytes=LIMIT
        ),
    )(measures, row_keys.reshape(1, rows), heavy_keys.reshape(1, heavy), table)
    result, report, slot_rows = pl.pallas_call(
        functools.partial(join, cfg),
        out_shape=(
            shaped(key_dev, columns, dtype=BF16),
            shaped(each, columns, dtype=BF16),
            shaped(key_rows, LANES),
        ),
        in_specs=[SMEM] + [VMEM] * 7,
        out_specs=(VMEM,) * 3,
        scratch_shapes=[pltpu.VMEM((key_dev, LANES), F32)],
        compiler_params=pltpu.CompilerParams(vmem_limit_bytes=LIMIT),
    )(heavy_keys, got, scales, heads, total, slots, orders, table)
    return (result, report, slot_rows.reshape(key_dev))


def solution(mesh):
    return jax.shard_map(
        body,
        mesh=mesh,
        in_specs=(P(("gx", "gy"), None), P(("gx", "gy")), P(("gx", "gy"), None), P(), P()),
        out_specs=(P(("gx", "gy"), None), P(("gx", "gy"), None), P(("gx", "gy"))),
        check_vma=False,
    )
```

```python
import functools

import jax
import jax.numpy as jnp
from jax import lax
from jax.experimental import pallas as pl
from jax.experimental.pallas import tpu as pltpu
from jax.sharding import PartitionSpec as P

MESH = pl.DeviceIdType.MESH
LANES = 128
LEAST = -3.4028235e38
F32 = jnp.float32
BF16 = jnp.bfloat16
VMEM = pl.BlockSpec(memory_space=pltpu.VMEM)
ANY = pl.BlockSpec(memory_space=pl.ANY)
SMEM = pl.BlockSpec(memory_space=pltpu.SMEM)
LIMIT = 60 * 1024 * 1024
NN = (((1,), (0,)), ((), ()))
NT = (((1,), (1,)), ((), ()))


def dot(a, b, dims=NN):
    return lax.dot_general(a, b, dims, preferred_element_type=F32)


def iota(shape, dim):
    return lax.broadcasted_iota(jnp.int32, shape, dim)


def onehot(mask):
    return jnp.where(mask, 1.0, 0.0).astype(BF16)


def group_rank(flags, group_rows):
    rows = flags.shape[0]
    lane_r, lane_c = iota((LANES, LANES), 0), iota((LANES, LANES), 1)
    inside = dot(flags, onehot(lane_r < lane_c))
    whole = dot(flags, onehot(lane_r >= 0))
    row_r, row_c = iota((rows, rows), 0), iota((rows, rows), 1)
    earlier = onehot((row_c < row_r) & (row_r // group_rows == row_c // group_rows))
    return inside + dot(earlier, whole.astype(BF16))


def split(values):
    high = values.astype(BF16)
    low = (values - high.astype(F32)).astype(BF16)
    return jnp.concatenate([high, low], axis=1)


def eye(rows):
    return iota((rows, LANES), 0) == iota((rows, LANES), 1)


def encode(values):
    largest = jnp.max(jnp.abs(values), axis=1, keepdims=True)
    safe = jnp.maximum(largest, 1e-30)
    fixed = jnp.round(values * (1.0 / safe) * 32767.0).astype(jnp.int32).astype(jnp.int16)
    return fixed, jnp.sum(jnp.where(eye(values.shape[0]), safe, 0.0), axis=0, keepdims=True)


def decode(fixed, scale):
    column = jnp.sum(jnp.where(eye(fixed.shape[0]), scale, 0.0), axis=1, keepdims=True)
    return fixed.astype(jnp.int32).astype(F32) * (column * (1.0 / 32767.0))


def joined_chains(chains):
    return chains[0] + jnp.maximum(chains[1], LEAST)


def pieces(total):
    return [(at, min(LANES, total - at)) for at in range(0, total, LANES)]


def byte_table(table, parts):
    pieces = [((table >> (8 * p)) & 255).astype(F32).T for p in range(parts)]
    return jnp.concatenate(pieces, axis=0).astype(BF16)


def look_up(bytes_table, row_hot, column_mask, parts):
    wide = dot(bytes_table, row_hot)
    found = 0.0
    for p in range(parts):
        piece = wide[p * LANES : (p + 1) * LANES]
        found = found + float(256**p) * jnp.sum(
            jnp.where(column_mask, piece, 0.0), axis=0, keepdims=True
        )
    return found.astype(jnp.int32)


def byte_count(largest):
    return (int(largest).bit_length() + 7) // 8


def gather_rows(cfg, measures, keys, heavy, key_slot, send, tally, small, slots, sums):
    rows, block, nr = cfg["rows"], cfg["block"], cfg["nr"]
    segments, capacity = cfg["segments"], cfg["capacity"]
    slot_parts = byte_count(nr * LANES - 1)
    slot_bytes = byte_table(key_slot[...], slot_parts)
    hist_key = jnp.zeros((nr, LANES), F32)
    hist_slot = jnp.zeros((nr, LANES), F32)
    heavy_sum = jnp.zeros((cfg["heavy"], LANES), F32)
    for c in range(rows // block):
        span = slice(c * block, (c + 1) * block)
        key = keys[:, span]
        row_hot = onehot(iota((nr, block), 0) == key >> 7)
        column_mask = iota((LANES, block), 0) == (key & 127)
        hist_key = hist_key + dot(row_hot, onehot(column_mask), NT)
        heavy_hot = jnp.where(heavy[...] == key, 1.0, 0.0)
        is_heavy = jnp.max(heavy_hot, axis=0, keepdims=True) > 0.0
        heavy_sum = heavy_sum + dot(heavy_hot.astype(BF16), measures[span, :])
        slot = jnp.where(is_heavy, -1, look_up(slot_bytes, row_hot, column_mask, slot_parts))
        slots[:, span] = slot
        slot_row = onehot(iota((nr, block), 0) == slot >> 7)
        slot_column = onehot(iota((LANES, block), 0) == (slot & 127))
        hist_slot = hist_slot + dot(slot_row, slot_column, NT)
    present = hist_slot > 0.0
    group = cfg["own"] // LANES
    tally[...] = jnp.zeros(tally.shape, F32)
    for x in range(cfg["gx"]):
        tally[x, 0:group, :] = hist_slot[x * group : (x + 1) * group]
    rank = group_rank(onehot(present), group).astype(jnp.int32)
    owner = iota((nr, LANES), 0) // group
    segment_table = jnp.where(present, owner * capacity + rank + 1, 0)
    seg_parts = byte_count(segments)
    segment_bytes = byte_table(segment_table, seg_parts)
    step = cfg["seg_block"]
    for c in range(rows // block):
        span = slice(c * block, (c + 1) * block)
        slot = slots[:, span]
        slot_row = onehot(iota((nr, block), 0) == slot >> 7)
        slot_mask = iota((LANES, block), 0) == (slot & 127)
        segment = look_up(segment_bytes, slot_row, slot_mask, seg_parts) - 1
        for s in range(segments // step):
            hot = onehot(iota((step, block), 0) == segment - s * step)
            product = dot(hot, measures[span, :])
            place = slice(s * step, (s + 1) * step)
            if c == 0:
                sums[place, :] = product
            else:
                sums[place, :] += product
    for x in range(cfg["gx"]):
        for p, (at, size) in enumerate(pieces(capacity)):
            first = x * capacity + at
            fixed, scale = encode(sums[first : first + size, :])
            send[x, at : at + size, :] = fixed
            tally[x, group + p : group + p + 1, :] = scale
    each, key_rows, height = cfg["heavy_each"], cfg["key_rows"], cfg["height"]
    small[...] = jnp.zeros(small.shape, F32)
    for d in range(cfg["devices"]):
        small[d * height : d * height + each, :] = heavy_sum[d * each : (d + 1) * each]
        top = (d + 1) * height
        small[top - key_rows : top, :] = hist_key[d * key_rows : (d + 1) * key_rows]


def place_rows(cfg, got, got_tally, key_slot, send, scales, tally, spread, ranks):
    gx, gy, own, kpp = cfg["gx"], cfg["gy"], cfg["own"], cfg["kpp"]
    key_rows, capacity = cfg["key_rows"], cfg["capacity"]
    group = own // LANES
    base = lax.axis_index("gx") * own
    local = key_slot[...] - base
    mine = (local >= 0) & (local < own)
    rank = jnp.where(mine, group_rank(onehot(mine), key_rows), -1.0).astype(jnp.int32)
    local = local.astype(F32)
    for y in range(gy):
        for x in range(gx):
            first = (x * gy + y) * key_rows
            acc = jnp.zeros((kpp, LANES), F32)
            for j in range(key_rows):
                hit = iota((kpp, LANES), 0) == rank[first + j : first + j + 1]
                acc = acc + jnp.where(hit, local[first + j : first + j + 1], 0.0)
            at = (y * gx + x) * kpp
            spread[at : at + kpp, :] = acc
    counts = jnp.concatenate([got_tally[i, 0:group, :] for i in range(gx)], axis=0)
    present = counts > 0.0
    ranks[...] = jnp.where(present, group_rank(onehot(present), group) + 1.0, 0.0)
    total = counts[0:group]
    for i in range(1, gx):
        total = total + counts[i * group : (i + 1) * group]
    tally[...] = total
    values = []
    for i in range(gx):
        decoded = [
            decode(got[i, at : at + size, :], got_tally[i, group + p : group + p + 1, :])
            for p, (at, size) in enumerate(pieces(capacity))
        ]
        values.append(split(jnp.concatenate(decoded, axis=0)))
    quarter = own // gy
    for q in range(gy):
        at = slice(q * quarter, (q + 1) * quarter)
        slot = jnp.sum(spread[at, :], axis=1, keepdims=True).astype(jnp.int32) - q * quarter
        found = jnp.zeros((quarter, gx), F32)
        for j in range(key_rows):
            hot = onehot(slot - j * LANES == iota((quarter, LANES), 1))
            table = ranks[pl.ds(q * key_rows + j, gx, stride=group), :].astype(BF16)
            found = found + dot(hot, table, NT)
        found = found.astype(jnp.int32) - 1
        out = jnp.zeros((quarter, 2 * LANES), F32)
        for i in range(gx):
            hot = onehot(found[:, i : i + 1] == iota((quarter, capacity), 1))
            out = out + dot(hot, values[i])
        out = out[:, :LANES] + out[:, LANES:]
        for x in range(gx):
            fixed, scale = encode(out[x * kpp : (x + 1) * kpp])
            send[q * gx + x] = fixed
            scales[q * gx + x] = scale


def join_rows(cfg, heavy, got, got_scales, got_small, got_tally, orders, key_slot, result, report, slot_rows, sums, joined):
    gx, gy, own, kpp = cfg["gx"], cfg["gy"], cfg["own"], cfg["kpp"]
    key_rows, height, each = cfg["key_rows"], cfg["height"], cfg["heavy_each"]
    key_dev = key_rows * LANES
    device = lax.axis_index("gx") * gy + lax.axis_index("gy")
    total = got_tally[0:key_rows]
    for y in range(1, gy):
        total = total + got_tally[y * key_rows : (y + 1) * key_rows]
    slot_rows[...] = total
    small = got_small[0:height]
    for d in range(1, cfg["devices"]):
        small = small + got_small[d * height : (d + 1) * height]
    for x in range(gx):
        part = decode(got[x * gy], got_scales[x * gy])
        for y in range(1, gy):
            part = part + decode(got[x * gy + y], got_scales[x * gy + y])
        sums[x * kpp : (x + 1) * kpp, :] = part
    values = split(sums[...])
    owner = key_slot[pl.ds(device * key_rows, key_rows), :] // own
    flags = jnp.concatenate([jnp.where(owner == x, 1.0, 0.0) for x in range(gx)], axis=0)
    rank = group_rank(flags.astype(BF16), key_rows)
    place = jnp.zeros((key_rows, LANES), F32)
    for x in range(gx):
        here = rank[x * key_rows : (x + 1) * key_rows] + float(x * kpp)
        place = place + jnp.where(owner == x, here, 0.0)
    counts = small[height - key_rows : height]
    stacked = jnp.concatenate([place, counts], axis=0)
    columns = stacked.T
    for j in range(key_rows):
        at = slice(j * LANES, (j + 1) * LANES)
        where = columns[:, j : j + 1].astype(jnp.int32)
        hot = onehot(where == iota((LANES, key_dev), 1))
        both = dot(hot, values)
        found = both[:, :LANES] + both[:, LANES:]
        for h in range(each):
            spot = heavy[device * each + h] - device * key_dev - j * LANES
            found = found + jnp.where(iota((LANES, LANES), 0) == spot, small[h : h + 1], 0.0)
        scale = lax.rsqrt(1.0 + columns[:, key_rows + j : key_rows + j + 1])
        value = orders[at, :].astype(F32) * found * scale
        joined[at, :] = value
        result[at, :] = value.astype(BF16)
    lines = [
        joined[pl.ds(heavy[device * each + h] - device * key_dev, 1), :] for h in range(each)
    ]
    report[...] = jnp.concatenate(lines, axis=0).astype(BF16)


def all_barrier(gx, gy, me_x, me_y):
    barrier = pltpu.get_barrier_semaphore()
    device = me_x * gy + me_y
    devices = gx * gy

    @pl.loop(1, devices)
    def _(step):
        other = lax.rem(device + step, devices)
        target = (other // gy, lax.rem(other, gy))
        pl.semaphore_signal(barrier, inc=1, device_id=target, device_id_type=MESH)

    pl.semaphore_wait(barrier, devices - 1)


def exchange(me, count, moves, address):
    for source, landing, send_sem, recv_sem, local_sem in moves:
        pltpu.make_async_copy(source(me), landing(me), local_sem).start()

    def remote(other, move):
        source, landing, send_sem, recv_sem, local_sem = move
        return pltpu.make_async_remote_copy(
            src_ref=source(other),
            dst_ref=landing(me),
            send_sem=send_sem.at[other],
            recv_sem=recv_sem.at[me],
            device_id=address(other),
            device_id_type=MESH,
        )

    def finish(other, move):
        source, landing, send_sem, recv_sem, local_sem = move
        copy = pltpu.make_async_remote_copy(
            src_ref=source(other),
            dst_ref=landing(other),
            send_sem=send_sem.at[other],
            recv_sem=recv_sem.at[other],
            device_id=address(other),
            device_id_type=MESH,
        )
        copy.wait_send()
        copy.wait_recv()

    @pl.loop(1, count)
    def _(step):
        for move in moves:
            remote(lax.rem(me + step, count), move).start()

    def end():
        @pl.loop(1, count)
        def _(step):
            for move in moves:
                finish(lax.rem(me + step, count), move)

        for source, landing, send_sem, recv_sem, local_sem in moves:
            pltpu.make_async_copy(source(me), landing(me), local_sem).wait()

    return end


def to_owners(gx, gy, send, tally, small, got, got_tally, got_small, sem_a, sem_b, sem_c, sem_d, sem_e, sem_f, local):
    me_x, me_y = lax.axis_index("gx"), lax.axis_index("gy")
    all_barrier(gx, gy, me_x, me_y)
    rows = (lambda i: send.at[i], lambda i: got.at[i], sem_a, sem_b, local.at[0])
    tallies = (lambda i: tally.at[i], lambda i: got_tally.at[i], sem_c, sem_d, local.at[1])
    end_x = exchange(me_x, gx, [rows, tallies], lambda i: (i, me_y))
    others = (lambda i: small.at[i], lambda i: got_small.at[i], sem_e, sem_f, local.at[2])
    end_all = exchange(
        me_x * gy + me_y, gx * gy, [others], lambda i: (i // gy, lax.rem(i, gy))
    )
    end_x()
    end_all()


def to_ranges(gx, gy, send, scales, tally, got, got_scales, got_tally, sem_a, sem_b, sem_c, sem_d, sem_e, sem_f, local):
    me_x, me_y = lax.axis_index("gx"), lax.axis_index("gy")
    all_barrier(gx, gy, me_x, me_y)
    rows = (
        lambda i: send.at[lax.rem(i, gy) * gx + i // gy],
        lambda i: got.at[i],
        sem_a,
        sem_b,
        local.at[0],
    )
    factors = (
        lambda i: scales.at[lax.rem(i, gy) * gx + i // gy],
        lambda i: got_scales.at[i],
        sem_e,
        sem_f,
        local.at[2],
    )
    end_all = exchange(
        me_x * gy + me_y, gx * gy, [rows, factors], lambda i: (i // gy, lax.rem(i, gy))
    )
    tallies = (lambda i: tally.at[i], lambda i: got_tally.at[i], sem_c, sem_d, local.at[1])
    end_y = exchange(me_y, gy, [tallies], lambda i: (me_x, i))
    end_y()
    end_all()


def shaped(*dims, dtype=F32):
    return jax.ShapeDtypeStruct(dims, dtype)


def split_body(measures, row_keys, orders, heavy_keys, key_slot):
    rows, columns = measures.shape
    gx, gy = lax.axis_size("gx"), lax.axis_size("gy")
    devices = gx * gy
    key_dev = orders.shape[0]
    key_rows = key_dev // LANES
    own = key_dev * gy
    nr = key_slot.shape[0] // LANES
    heavy = heavy_keys.shape[0]
    each = heavy // devices
    capacity = max(rows // 32, 3 * rows // (4 * gx)) // 4
    segments = gx * capacity
    cfg = dict(
        rows=rows,
        block=min(rows, 2048),
        nr=nr,
        gx=gx,
        gy=gy,
        devices=devices,
        own=own,
        kpp=key_dev // gx,
        key_rows=key_rows,
        heavy=heavy,
        heavy_each=each,
        height=-(-(each + key_rows) // 8) * 8,
        capacity=capacity,
        segments=segments,
        seg_block=512 if segments % 512 == 0 else segments,
    )
    height = cfg["height"]
    group = own // LANES
    params = pltpu.CompilerParams(vmem_limit_bytes=LIMIT)
    table = key_slot.reshape(nr, LANES)
    kpp = cfg["kpp"]
    tall = group + -(-len(pieces(capacity)) // 8) * 8
    send, tally, small = pl.pallas_call(
        functools.partial(gather_rows, cfg),
        out_shape=(
            shaped(gx, capacity, columns, dtype=jnp.int16),
            shaped(gx, tall, LANES),
            shaped(devices * height, LANES),
        ),
        in_specs=[VMEM] * 4,
        out_specs=(VMEM,) * 3,
        scratch_shapes=[pltpu.VMEM((1, rows), jnp.int32), pltpu.VMEM((segments, columns), F32)],
        compiler_params=params,
    )(measures, row_keys.reshape(1, rows), heavy_keys.reshape(heavy, 1), table)
    dma = pltpu.SemaphoreType.DMA
    got, got_tally, got_small = pl.pallas_call(
        functools.partial(to_owners, gx, gy),
        out_shape=(
            shaped(gx, capacity, columns, dtype=jnp.int16),
            shaped(gx, tall, LANES),
            shaped(devices, height, LANES),
        ),
        in_specs=[ANY] * 3,
        out_specs=(ANY,) * 3,
        scratch_shapes=[dma((gx,))] * 4 + [dma((devices,))] * 2 + [dma((3,))],
        compiler_params=pltpu.CompilerParams(collective_id=0, has_side_effects=True),
    )(send, tally, small.reshape(devices, height, LANES))
    send2, scales2, tally2 = pl.pallas_call(
        functools.partial(place_rows, cfg),
        out_shape=(
            shaped(devices, kpp, columns, dtype=jnp.int16),
            shaped(devices, 1, LANES),
            shaped(group, LANES),
        ),
        in_specs=[VMEM] * 3,
        out_specs=(VMEM,) * 3,
        scratch_shapes=[pltpu.VMEM((own, LANES), F32), pltpu.VMEM((gx * group, LANES), F32)],
        compiler_params=params,
    )(got, got_tally, table)
    got2, got_scales2, got_tally2 = pl.pallas_call(
        functools.partial(to_ranges, gx, gy),
        out_shape=(
            shaped(devices, kpp, columns, dtype=jnp.int16),
            shaped(devices, 1, LANES),
            shaped(gy, key_rows, LANES),
        ),
        in_specs=[ANY] * 3,
        out_specs=(ANY,) * 3,
        scratch_shapes=[dma((devices,))] * 2
        + [dma((gy,))] * 2
        + [dma((devices,))] * 2
        + [dma((3,))],
        compiler_params=pltpu.CompilerParams(collective_id=1, has_side_effects=True),
    )(send2, scales2, tally2.reshape(gy, key_rows, LANES))
    result, report, slot_rows = pl.pallas_call(
        functools.partial(join_rows, cfg),
        out_shape=(
            shaped(key_dev, columns, dtype=BF16),
            shaped(each, columns, dtype=BF16),
            shaped(key_rows, LANES),
        ),
        in_specs=[SMEM] + [VMEM] * 6,
        out_specs=(VMEM,) * 3,
        scratch_shapes=[pltpu.VMEM((key_dev, LANES), F32)] * 2,
        compiler_params=params,
    )(
        heavy_keys,
        got2,
        got_scales2,
        got_small.reshape(devices * height, LANES),
        got_tally2.reshape(gy * key_rows, LANES),
        orders,
        table,
    )
    return (result, report, slot_rows.reshape(key_dev))


def fused(
    cfg, measures, keys_hbm, heavy_hbm, table_hbm,
    got2, scales2, hgot, side_out,
    keys, heavy, table, side, rows_in, pair, parity, seg_hot, group_row, local_row, hist, hist16, send1, got1, goth, cnt_got,
    codes, ranks, found, wide, hsend, send2, srow, tsend, tgot,
    load_sem, in_sem, out_sem, back_sem, row_sem, own_sem,
):
    gx, gy, nr, rows, block = cfg["gx"], cfg["gy"], cfg["nr"], cfg["rows"], cfg["block"]
    devices, own, kpp, key_rows = cfg["devices"], cfg["own"], cfg["kpp"], cfg["key_rows"]
    cap, extra, seg, deep = cfg["cap"], cfg["extra"], cfg["seg"], cfg["deep"]
    each, planes, half_seg = cfg["each"], cfg["planes"], cfg["seg"] // 2
    used, at_once = (cap + extra) // 2, cfg["at_once"]
    key_dev = key_rows * LANES
    per_tile = LANES // kpp
    mx, my = lax.axis_index("gx"), lax.axis_index("gy")
    me = mx * gy + my
    z, j = me // gx, lax.rem(me, gx)

    def remote(src, dst, send_sem, recv_sem, where):
        return pltpu.make_async_remote_copy(
            src_ref=src, dst_ref=dst, send_sem=send_sem, recv_sem=recv_sem,
            device_id=where, device_id_type=MESH,
        )

    def in_plane(p, x):
        d = p * gx + x
        return (d // gy, lax.rem(d, gy))

    beside = [lax.rem(my + s, gy) for s in range(gy)]

    def every_other(act):
        for y in beside[1:]:
            act(mx * gy + y, (mx, y))

        @pl.loop(1, gx)
        def _(s):
            x = lax.rem(mx + s, gx)
            for y in beside:
                act(x * gy + y, (x, y))

    self_id = (mx, my)
    others = devices - 1
    COUNTS, HISTS, ROWS, MERGED, SCALES, HEADS, TOTALS = range(7)

    loads = [
        pltpu.make_async_copy(source, target, in_sem.at[i])
        for i, (source, target) in enumerate(
            [(keys_hbm, keys), (heavy_hbm, heavy), (table_hbm, table)]
        )
    ]
    for one in loads:
        one.start()
    load = pltpu.make_async_copy(measures, rows_in, load_sem)
    load.start()

    barrier = pltpu.get_barrier_semaphore()

    every_other(
        lambda d, where: pl.semaphore_signal(
            barrier, inc=1, device_id=where, device_id_type=MESH
        )
    )
    for one in loads:
        one.wait()

    chains = [jnp.zeros((nr, LANES), F32)] * 2
    for c in range(rows // block):
        span = slice(c * block, (c + 1) * block)
        key = keys[:, span]
        row_hot = onehot(iota((nr, block), 0) == key >> 7)
        seg_hot[:, span] = row_hot
        column_hot = onehot(iota((LANES, block), 0) == (key & 127))
        chains[c % 2] = chains[c % 2] + dot(row_hot, column_hot, NT)
    total = joined_chains(chains)
    hist[...] = total.reshape(devices, key_rows, LANES)
    hist16[...] = total.astype(jnp.int32).astype(jnp.int16)
    cnt_got[me] = hist[me]

    owner = table[...] // own
    heavy_key = heavy[...]
    heads = heavy_key.shape[1]
    code = iota((1, heads), 1) + 1
    row_of = iota((nr, heads), 0) == heavy_key >> 7
    col_of = onehot(iota((LANES, heads), 0) == (heavy_key & 127))
    low = dot(jnp.where(row_of, (code & 127).astype(F32), 0.0).astype(BF16), col_of, NT)
    high = dot(jnp.where(row_of, (code >> 7).astype(F32), 0.0).astype(BF16), col_of, NT)
    which = (low + 128.0 * high).astype(jnp.int32)
    codes[...] = which.astype(F32).reshape(devices, key_rows, LANES)
    light = which == 0
    present = (total > 0.0) & light
    lane_r, lane_c = iota((LANES, 2 * LANES), 0), iota((LANES, 2 * LANES), 1)
    upper = onehot((lane_c >= LANES) | (lane_r < lane_c))
    lower = onehot(iota((nr, nr), 1) < iota((nr, nr), 0))
    flags = jnp.concatenate(
        [jnp.where(present & (owner == x), 1.0, 0.0) for x in range(gx)], axis=0
    ).astype(BF16)
    both = dot(flags, upper)
    local = jnp.zeros((nr, LANES), F32)
    for x in range(gx):
        part = both[x * nr : (x + 1) * nr]
        rank = part[:, :LANES] + dot(lower, part[:, LANES:].astype(BF16))
        local = local + jnp.where(owner == x, rank, 0.0)
    head = which - 1
    block_of = head // each
    group = jnp.where(light, owner, lax.rem(block_of, gx))
    local = jnp.where(
        light, local, (cap + (block_of // gx) * each + lax.rem(head, each)).astype(F32)
    )
    tables = jnp.concatenate([group.astype(F32).T, local.T], axis=0).astype(BF16)
    for c in range(rows // block):
        span = slice(c * block, (c + 1) * block)
        spread = dot(tables, seg_hot[:, span])
        mask = iota((LANES, block), 0) == (keys[:, span] & 127)
        group_row[:, span] = jnp.sum(
            jnp.where(mask, spread[:LANES], 0.0), axis=0, keepdims=True
        ).astype(jnp.int32)
        inside = jnp.sum(
            jnp.where(mask, spread[LANES:], 0.0), axis=0, keepdims=True
        ).astype(jnp.int32)
        local_row[:, span] = inside >> 1
        odd = (inside & 1).astype(F32)
        for i in range(block // LANES):
            at = c * (block // LANES) + i
            parity[at : at + 1, :] = odd[:, i * LANES : (i + 1) * LANES]

    pl.semaphore_wait(barrier, devices - 1)

    @pl.loop(0, gx - 1)
    def _(s):
        x = lax.rem(j + 1 + s, gx)
        t = lax.rem(2 * gx - 2 - s, gx)
        remote(hist16, goth.at[t], out_sem.at[HISTS], back_sem.at[HISTS], in_plane(z, x)).start()

    every_other(
        lambda d, where: remote(
            hist.at[d], cnt_got.at[me], out_sem.at[COUNTS], back_sem.at[COUNTS], where
        ).start()
    )

    load.wait()
    turned = parity[...].T
    for c in range(rows // LANES):
        span = slice(c * LANES, (c + 1) * LANES)
        line = rows_in[span, :]
        odd = line * jnp.broadcast_to(turned[:, c : c + 1], (LANES, LANES)).astype(BF16)
        pair[span, LANES:] = odd
        pair[span, :LANES] = line - odd

    def encode(values):
        largest = jnp.max(jnp.abs(values), axis=1, keepdims=True)
        power = jnp.floor(jnp.log2(jnp.maximum(largest, 1e-30))) + 1.0
        fixed = jnp.clip(jnp.round(values * jnp.exp2(15.0 - power)), -32767.0, 32767.0)
        return fixed, power

    for first in range(0, gx, at_once):
        steps = range(first, first + at_once)
        chains = [jnp.zeros((at_once * half_seg, 2 * LANES), F32)] * 2
        for c in range(rows // block):
            span = slice(c * block, (c + 1) * block)
            group, local = group_row[:, span], local_row[:, span]
            hot = [
                jnp.where(
                    iota((half_seg, block), 0)
                    == jnp.where(group == lax.rem(j + 1 + s, gx), local, -1),
                    1.0,
                    0.0,
                )
                for s in steps
            ]
            chains[c % 2] = chains[c % 2] + dot(
                jnp.concatenate(hot, axis=0).astype(BF16), pair[span, :]
            )
        acc = joined_chains(chains)
        for s in steps:
            at = (s - first) * half_seg
            both = acc[at : at + half_seg]
            fixed, power = encode(jnp.concatenate([both[:, :LANES], both[:, LANES:]], axis=0))
            lines = []
            for top, size in pieces(seg):
                diagonal = iota((size, LANES), 0) == iota((size, LANES), 1)
                lines.append(
                    jnp.sum(jnp.where(diagonal, power[top : top + size], 0.0), axis=0, keepdims=True)
                )
            foot = jnp.zeros((half_seg - used, LANES), F32)
            for n, one in enumerate(lines):
                foot = jnp.where(iota(foot.shape, 0) == n, one, foot)
            whole = jnp.concatenate([fixed[:used], foot, fixed[half_seg:]], axis=0)
            send1[s] = whole.astype(jnp.int32).astype(jnp.int16)
            if s < gx - 1:
                t = (2 * gx - 2 - s) % gx
                remote(
                    send1.at[s], got1.at[t], out_sem.at[ROWS], row_sem.at[t],
                    in_plane(z, lax.rem(j + 1 + s, gx)),
                ).start()

    def all_of(ref, kind, number):
        return remote(
            ref.at[0:number], ref.at[0:number], out_sem.at[kind], back_sem.at[kind], self_id
        )

    all_of(goth, HISTS, gx - 1).wait_recv()
    mine = (owner == j) & light
    arrived = []
    for t in range(gx):
        here = hist16[...] if t == gx - 1 else goth[t]
        arrived.append(jnp.where((here.astype(jnp.int32) > 0) & mine, 1.0, 0.0))
    flags = jnp.concatenate(arrived, axis=0)
    both = dot(flags.astype(BF16), upper)
    for t in range(gx):
        part = both[t * nr : (t + 1) * nr]
        rank = (part[:, :LANES] + dot(lower, part[:, LANES:].astype(BF16))).astype(jnp.int32)
        rank = ((rank >> 1) + (rank & 1) * half_seg + 1).astype(F32)
        ranks[t * nr : (t + 1) * nr, :] = rank * flags[t * nr : (t + 1) * nr]
    own_flags = onehot(owner == j)
    both = dot(own_flags, upper)
    row_r, row_c = iota((nr, nr), 0), iota((nr, nr), 1)
    near = onehot((row_c < row_r) & (row_r // key_rows == row_c // key_rows))
    rank = both[:, :LANES] + dot(near, both[:, LANES:].astype(BF16))
    rank = jnp.where(owner == j, rank, -1.0).astype(jnp.int32)
    for d in range(devices):
        hot, tall = [], []
        for q in range(key_rows):
            r = d * key_rows + q
            hot.append(onehot(iota((kpp, LANES), 0) == rank[r : r + 1]))
            tall.append(ranks[pl.ds(r, gx, stride=nr), :].astype(BF16))
        found[d * kpp : (d + 1) * kpp, 0:gx] = dot(
            jnp.concatenate(hot, axis=1), jnp.concatenate(tall, axis=1), NT
        )

    all_of(cnt_got, COUNTS, others).wait()

    counted = cnt_got[0]
    for d in range(1, devices):
        counted = counted + cnt_got[d]
    side[key_rows : 2 * key_rows, :] = counted
    tsend[...] = jnp.where(codes[me] == 0.0, counted, 0.0)
    tgot[mx] = tsend[...]

    @pl.loop(1, gx)
    def _(s):
        x = lax.rem(mx + s, gx)
        remote(tsend, tgot.at[mx], out_sem.at[TOTALS], back_sem.at[TOTALS], (x, my)).start()

    heads_sum = [jnp.zeros((extra // 2, LANES), F32)] * 2
    powers = []
    for t in range(gx):
        if t < gx - 1:
            remote(send1.at[t], got1.at[t], out_sem.at[ROWS], row_sem.at[t], self_id).wait_recv()
            block16 = got1[t]
        else:
            block16 = send1[t]
        value = block16.astype(jnp.int32)
        wide[t, 0:seg, :LANES] = (value >> 8).astype(F32).astype(BF16)
        wide[t, 0:seg, LANES:] = (value & 255).astype(F32).astype(BF16)
        if deep > seg:
            wide[t, seg:deep, :] = jnp.zeros((deep - seg, 2 * LANES), BF16)
        scale = jnp.exp2(value[used : used + len(pieces(seg))].astype(F32) - 15.0)
        powers.append(
            jnp.concatenate([scale[p : p + 1] for p in range(deep // LANES)], axis=1)
        )
        for b in range(2):
            top = b * half_seg + cap // 2
            p, at = top // LANES, top % LANES
            column = jnp.sum(
                jnp.where(
                    iota((extra // 2, LANES), 1) == iota((extra // 2, LANES), 0) + at,
                    scale[p : p + 1],
                    0.0,
                ),
                axis=1, keepdims=True,
            )
            heads_sum[b] = heads_sum[b] + value[top : top + extra // 2].astype(F32) * column
    hsend[...] = jnp.concatenate(heads_sum, axis=0)

    local_heads = pltpu.make_async_copy(hsend, hgot.at[z], own_sem.at[0])
    local_heads.start()

    @pl.loop(1, planes)
    def _(s):
        other = lax.rem(z + s, planes)
        remote(
            hsend, hgot.at[z], out_sem.at[HEADS], back_sem.at[HEADS], in_plane(other, j)
        ).start()

    chunk = gx * kpp
    shift = lax.rem(j, per_tile) * kpp
    half = planes // 2
    lanes = (iota((1, deep), 1) + 1).astype(F32)
    if planes == 4:
        order = [
            lax.rem(z + half, planes), planes - 1 - z,
            planes - 1 - lax.rem(z + half, planes), z,
        ]
    else:
        order = [lax.rem(z + s, planes) for s in range(1, planes + 1)]
    for c in range(planes):
        far = order[c]
        spot = found[pl.ds(pl.multiple_of(far * chunk, chunk), chunk), :]
        chains = [jnp.zeros((chunk, 2 * LANES), F32)] * 2
        for t in range(gx):
            hit = spot[:, t : t + 1] == lanes
            chains[t % 2] = chains[t % 2] + dot(
                jnp.where(hit, powers[t], 0.0).astype(BF16), wide[t]
            )
        acc = joined_chains(chains)
        fixed, power = encode(acc[:, :LANES] * 256.0 + acc[:, LANES:])
        send2[c] = fixed.astype(jnp.int32).astype(jnp.int16).reshape(gx, kpp, LANES)
        scale = jnp.exp2(power - 15.0)
        diagonal = iota((kpp, LANES), 1) == iota((kpp, LANES), 0) + shift
        for x in range(gx):
            srow[c, x] = jnp.sum(
                jnp.where(diagonal, scale[x * kpp : (x + 1) * kpp], 0.0), axis=0, keepdims=True
            )
        last = c == planes - 1

        @pl.loop(0, gx - 1 if last else gx)
        def _(s):
            x = lax.rem(j + 1 + s, gx)
            where = in_plane(far, x)
            remote(
                send2.at[c, x], got2.at[me], out_sem.at[MERGED], back_sem.at[MERGED], where
            ).start()
            remote(
                srow.at[c, x], scales2.at[me], out_sem.at[SCALES], back_sem.at[SCALES], where
            ).start()

        if last:
            keep = pltpu.make_async_copy(send2.at[c, j], got2.at[me], own_sem.at[1])
            keep.start()
            keep_row = pltpu.make_async_copy(srow.at[c, j], scales2.at[me], own_sem.at[2])
            keep_row.start()

    all_of(tgot, TOTALS, gx - 1).wait()

    base = me * key_dev
    left, right = [], []
    for m in range(gx):
        slots = table[pl.ds((m * gy + my) * key_rows, key_rows), :] - base
        for q in range(key_rows):
            line = slots[q : q + 1]
            amount = tgot[m, q : q + 1, :].astype(jnp.int32)
            bands = [
                jnp.where(
                    iota((8, LANES), 0) == (line >> 7), ((amount >> (8 * b)) & 255).astype(F32), 0.0
                )
                for b in range(3)
            ]
            left.append(jnp.concatenate(bands + [jnp.zeros((8, LANES), F32)], axis=0).astype(BF16))
            right.append(onehot(iota((LANES, LANES), 0) == (line & 127)))
    middle = len(left) // 2
    bands = joined_chains(
        [
            dot(jnp.concatenate(left[part], axis=1), jnp.concatenate(right[part], axis=1), NT)
            for part in (slice(0, middle), slice(middle, None))
        ]
    )
    side[2 * key_rows : 3 * key_rows, :] = (
        bands[0:8] + 256.0 * bands[8:16] + 65536.0 * bands[16:24]
    )[0:key_rows]
    owner = table[pl.ds(me * key_rows, key_rows), :] // own
    flags = jnp.concatenate([jnp.where(owner == x, 1.0, 0.0) for x in range(gx)], axis=0)
    rank = group_rank(flags.astype(BF16), key_rows)
    place = jnp.zeros((key_rows, LANES), F32)
    for x in range(gx):
        inside = rank[x * key_rows : (x + 1) * key_rows] + float(x * kpp)
        place = place + jnp.where(owner == x, inside, 0.0)
    side[0:key_rows, :] = place
    hand_over = pltpu.make_async_copy(side, side_out, own_sem.at[3])
    hand_over.start()

    all_of(goth, HISTS, gx - 1).wait_send()
    all_of(send1, ROWS, gx - 1).wait_send()
    local_heads.wait()
    keep.wait()
    keep_row.wait()
    hand_over.wait()
    all_of(hgot, HEADS, planes - 1).wait()
    all_of(got2, MERGED, others).wait()
    all_of(scales2, SCALES, others).wait()


def join(
    cfg, heavy, got_hbm, scales_hbm, heads_hbm, side_hbm, orders_hbm, result, report, slot_rows,
    joined, got, scales, heads, side, orders, sems,
):
    gx, gy, kpp = cfg["gx"], cfg["gy"], cfg["kpp"]
    key_rows, each, planes, extra = cfg["key_rows"], cfg["each"], cfg["planes"], cfg["extra"]
    key_dev = key_rows * LANES
    per_tile = LANES // kpp
    loads = [
        pltpu.make_async_copy(source, target, sems.at[i])
        for i, (source, target) in enumerate(
            [(got_hbm, got), (side_hbm, side), (scales_hbm, scales), (heads_hbm, heads), (orders_hbm, orders)]
        )
    ]
    for one in loads:
        one.start()
    device = lax.axis_index("gx") * gy + lax.axis_index("gy")
    z = device // gx
    for one in loads[1:4]:
        one.wait()
    slot_rows[...] = side[2 * key_rows : 3 * key_rows, :]
    small = heads[0]
    for p in range(1, planes):
        small = small + heads[p]
    spots = []
    for h in range(each):
        entry = z * each + h
        spots.append(lax.rem(entry, 2) * (extra // 2) + entry // 2)
    columns = side[0 : 2 * key_rows, :].T
    loads[0].wait()
    loads[4].wait()
    values, lines = [], []
    for p in range(planes):
        value = got[p * gx : (p + 1) * gx].reshape(key_dev, LANES).astype(jnp.int32)
        values.append(
            jnp.concatenate([(value >> 8).astype(F32), (value & 255).astype(F32)], axis=1).astype(BF16)
        )
        tiles = []
        for x in range(0, gx, per_tile):
            tile = scales[p * gx + x]
            for i in range(1, per_tile):
                tile = tile + scales[p * gx + x + i]
            tiles.append(tile)
        lines.append(jnp.concatenate(tiles, axis=1))
    for j in range(key_rows):
        at = slice(j * LANES, (j + 1) * LANES)
        hit = columns[:, j : j + 1].astype(jnp.int32) == iota((LANES, key_dev), 1)
        chains = [jnp.zeros((LANES, 2 * LANES), F32)] * 2
        for p in range(planes):
            chains[p % 2] = chains[p % 2] + dot(
                jnp.where(hit, lines[p], 0.0).astype(BF16), values[p]
            )
        both = joined_chains(chains)
        sums = both[:, :LANES] * 256.0 + both[:, LANES:]
        for h in range(each):
            spot = heavy[device * each + h] - device * key_dev - j * LANES
            line = jnp.sum(
                jnp.where(iota((extra, LANES), 0) == spots[h], small, 0.0), axis=0, keepdims=True
            )
            sums = sums + jnp.where(iota((LANES, LANES), 0) == spot, line, 0.0)
        scale = lax.rsqrt(1.0 + columns[:, key_rows + j : key_rows + j + 1])
        value = orders[at, :].astype(F32) * sums * scale
        joined[at, :] = value
        result[at, :] = value.astype(BF16)
    picked = [
        joined[pl.ds(heavy[device * each + h] - device * key_dev, 1), :] for h in range(each)
    ]
    report[...] = jnp.concatenate(picked, axis=0).astype(BF16)


def body(measures, row_keys, orders, heavy_keys, key_slot):
    rows, columns = measures.shape
    gx, gy = lax.axis_size("gx"), lax.axis_size("gy")
    devices = gx * gy
    key_dev = orders.shape[0]
    key_rows = key_dev // LANES
    nr = key_slot.shape[0] // LANES
    heavy = heavy_keys.shape[0]
    each = heavy // devices
    if gx * nr > 2048:
        return split_body(measures, row_keys, orders, heavy_keys, key_slot)
    planes = devices // gx
    cap = max(rows // 32, 3 * rows // (4 * gx)) // 4
    extra = planes * each
    seg = 2 * (-(-((cap + extra) // 2 + len(pieces(cap + extra + 16))) // 8) * 8)
    deep = -(-cap // LANES) * LANES
    kpp = key_dev // gx
    cfg = dict(
        rows=rows, block=min(rows, 2048), nr=nr, gx=gx, gy=gy, devices=devices,
        own=key_dev * gy, kpp=kpp, key_rows=key_rows, each=each, planes=planes,
        cap=cap, extra=extra, seg=seg, at_once=2 if gx % 2 == 0 else gx, deep=max(deep, -(-seg // LANES) * LANES),
    )
    deep = cfg["deep"]
    table = key_slot.reshape(nr, LANES)
    dma = pltpu.SemaphoreType.DMA
    i16 = jnp.int16
    got, scales, heads, side = pl.pallas_call(
        functools.partial(fused, cfg),
        out_shape=(
            shaped(devices, kpp, columns, dtype=i16),
            shaped(devices, 1, LANES),
            shaped(planes, extra, LANES),
            shaped(3 * key_rows, LANES),
        ),
        in_specs=[ANY] * 4,
        out_specs=(ANY,) * 4,
        scratch_shapes=[
            pltpu.VMEM((1, rows), jnp.int32),
            pltpu.VMEM((1, heavy), jnp.int32),
            pltpu.VMEM((nr, LANES), jnp.int32),
            pltpu.VMEM((3 * key_rows, LANES), F32),
            pltpu.VMEM((rows, columns), BF16),
            pltpu.VMEM((rows, 2 * columns), BF16),
            pltpu.VMEM((rows // LANES, LANES), F32),
            pltpu.VMEM((nr, rows), BF16),
            pltpu.VMEM((1, rows), jnp.int32),
            pltpu.VMEM((1, rows), jnp.int32),
            pltpu.VMEM((devices, key_rows, LANES), F32),
            pltpu.VMEM((nr, LANES), i16),
            pltpu.VMEM((gx, seg, LANES), i16),
            pltpu.VMEM((gx, seg, LANES), i16),
            pltpu.VMEM((gx, nr, LANES), i16),
            pltpu.VMEM((devices, key_rows, LANES), F32),
            pltpu.VMEM((devices, key_rows, LANES), F32),
            pltpu.VMEM((gx * nr, LANES), F32),
            pltpu.VMEM((devices * kpp, LANES), F32),
            pltpu.VMEM((gx, deep, 2 * LANES), BF16),
            pltpu.VMEM((extra, LANES), F32),
            pltpu.VMEM((planes, gx, kpp, LANES), i16),
            pltpu.VMEM((planes, gx, 1, LANES), F32),
            pltpu.VMEM((key_rows, LANES), F32),
            pltpu.VMEM((gx, key_rows, LANES), F32),
            dma,
            dma((3,)),
            dma((7,)),
            dma((7,)),
            dma((gx,)),
            dma((4,)),
        ],
        compiler_params=pltpu.CompilerParams(
            collective_id=2, has_side_effects=True, vmem_limit_bytes=LIMIT
        ),
    )(measures, row_keys.reshape(1, rows), heavy_keys.reshape(1, heavy), table)
    result, report, slot_rows = pl.pallas_call(
        functools.partial(join, cfg),
        out_shape=(
            shaped(key_dev, columns, dtype=BF16),
            shaped(each, columns, dtype=BF16),
            shaped(key_rows, LANES),
        ),
        in_specs=[SMEM] + [ANY] * 5,
        out_specs=(VMEM,) * 3,
        scratch_shapes=[
            pltpu.VMEM((key_dev, LANES), F32),
            pltpu.VMEM((devices, kpp, columns), i16),
            pltpu.VMEM((devices, 1, LANES), F32),
            pltpu.VMEM((planes, extra, LANES), F32),
            pltpu.VMEM((3 * key_rows, LANES), F32),
            pltpu.VMEM((key_dev, columns), BF16),
            dma((5,)),
        ],
        compiler_params=pltpu.CompilerParams(vmem_limit_bytes=LIMIT),
    )(heavy_keys, got, scales, heads, side, orders)
    return (result, report, slot_rows.reshape(key_dev))


def solution(mesh):
    return jax.shard_map(
        body,
        mesh=mesh,
        in_specs=(P(("gx", "gy"), None), P(("gx", "gy")), P(("gx", "gy"), None), P(), P()),
        out_specs=(P(("gx", "gy"), None), P(("gx", "gy"), None), P(("gx", "gy"))),
        check_vma=False,
    )
```

```python
import functools

import jax
import jax.numpy as jnp
from jax import lax
from jax.experimental import pallas as pl
from jax.experimental.pallas import tpu as pltpu
from jax.sharding import PartitionSpec as P

MESH = pl.DeviceIdType.MESH
LANES = 128
LEAST = -3.4028235e38
F32 = jnp.float32
BF16 = jnp.bfloat16
VMEM = pl.BlockSpec(memory_space=pltpu.VMEM)
ANY = pl.BlockSpec(memory_space=pl.ANY)
SMEM = pl.BlockSpec(memory_space=pltpu.SMEM)
LIMIT = 60 * 1024 * 1024
NN = (((1,), (0,)), ((), ()))
NT = (((1,), (1,)), ((), ()))


def dot(a, b, dims=NN):
    return lax.dot_general(a, b, dims, preferred_element_type=F32)


def iota(shape, dim):
    return lax.broadcasted_iota(jnp.int32, shape, dim)


def onehot(mask):
    return jnp.where(mask, 1.0, 0.0).astype(BF16)


def group_rank(flags, group_rows):
    rows = flags.shape[0]
    lane_r, lane_c = iota((LANES, LANES), 0), iota((LANES, LANES), 1)
    inside = dot(flags, onehot(lane_r < lane_c))
    whole = dot(flags, onehot(lane_r >= 0))
    row_r, row_c = iota((rows, rows), 0), iota((rows, rows), 1)
    earlier = onehot((row_c < row_r) & (row_r // group_rows == row_c // group_rows))
    return inside + dot(earlier, whole.astype(BF16))


def split(values):
    high = values.astype(BF16)
    low = (values - high.astype(F32)).astype(BF16)
    return jnp.concatenate([high, low], axis=1)


def eye(rows):
    return iota((rows, LANES), 0) == iota((rows, LANES), 1)


def encode(values):
    largest = jnp.max(jnp.abs(values), axis=1, keepdims=True)
    safe = jnp.maximum(largest, 1e-30)
    fixed = jnp.round(values * (1.0 / safe) * 32767.0).astype(jnp.int32).astype(jnp.int16)
    return fixed, jnp.sum(jnp.where(eye(values.shape[0]), safe, 0.0), axis=0, keepdims=True)


def decode(fixed, scale):
    column = jnp.sum(jnp.where(eye(fixed.shape[0]), scale, 0.0), axis=1, keepdims=True)
    return fixed.astype(jnp.int32).astype(F32) * (column * (1.0 / 32767.0))


def joined_chains(chains):
    return chains[0] + jnp.maximum(chains[1], LEAST)


def pieces(total):
    return [(at, min(LANES, total - at)) for at in range(0, total, LANES)]


def byte_table(table, parts):
    pieces = [((table >> (8 * p)) & 255).astype(F32).T for p in range(parts)]
    return jnp.concatenate(pieces, axis=0).astype(BF16)


def look_up(bytes_table, row_hot, column_mask, parts):
    wide = dot(bytes_table, row_hot)
    found = 0.0
    for p in range(parts):
        piece = wide[p * LANES : (p + 1) * LANES]
        found = found + float(256**p) * jnp.sum(
            jnp.where(column_mask, piece, 0.0), axis=0, keepdims=True
        )
    return found.astype(jnp.int32)


def byte_count(largest):
    return (int(largest).bit_length() + 7) // 8


def gather_rows(cfg, measures, keys, heavy, key_slot, send, tally, small, slots, sums):
    rows, block, nr = cfg["rows"], cfg["block"], cfg["nr"]
    segments, capacity = cfg["segments"], cfg["capacity"]
    slot_parts = byte_count(nr * LANES - 1)
    slot_bytes = byte_table(key_slot[...], slot_parts)
    hist_key = jnp.zeros((nr, LANES), F32)
    hist_slot = jnp.zeros((nr, LANES), F32)
    heavy_sum = jnp.zeros((cfg["heavy"], LANES), F32)
    for c in range(rows // block):
        span = slice(c * block, (c + 1) * block)
        key = keys[:, span]
        row_hot = onehot(iota((nr, block), 0) == key >> 7)
        column_mask = iota((LANES, block), 0) == (key & 127)
        hist_key = hist_key + dot(row_hot, onehot(column_mask), NT)
        heavy_hot = jnp.where(heavy[...] == key, 1.0, 0.0)
        is_heavy = jnp.max(heavy_hot, axis=0, keepdims=True) > 0.0
        heavy_sum = heavy_sum + dot(heavy_hot.astype(BF16), measures[span, :])
        slot = jnp.where(is_heavy, -1, look_up(slot_bytes, row_hot, column_mask, slot_parts))
        slots[:, span] = slot
        slot_row = onehot(iota((nr, block), 0) == slot >> 7)
        slot_column = onehot(iota((LANES, block), 0) == (slot & 127))
        hist_slot = hist_slot + dot(slot_row, slot_column, NT)
    present = hist_slot > 0.0
    group = cfg["own"] // LANES
    tally[...] = jnp.zeros(tally.shape, F32)
    for x in range(cfg["gx"]):
        tally[x, 0:group, :] = hist_slot[x * group : (x + 1) * group]
    rank = group_rank(onehot(present), group).astype(jnp.int32)
    owner = iota((nr, LANES), 0) // group
    segment_table = jnp.where(present, owner * capacity + rank + 1, 0)
    seg_parts = byte_count(segments)
    segment_bytes = byte_table(segment_table, seg_parts)
    step = cfg["seg_block"]
    for c in range(rows // block):
        span = slice(c * block, (c + 1) * block)
        slot = slots[:, span]
        slot_row = onehot(iota((nr, block), 0) == slot >> 7)
        slot_mask = iota((LANES, block), 0) == (slot & 127)
        segment = look_up(segment_bytes, slot_row, slot_mask, seg_parts) - 1
        for s in range(segments // step):
            hot = onehot(iota((step, block), 0) == segment - s * step)
            product = dot(hot, measures[span, :])
            place = slice(s * step, (s + 1) * step)
            if c == 0:
                sums[place, :] = product
            else:
                sums[place, :] += product
    for x in range(cfg["gx"]):
        for p, (at, size) in enumerate(pieces(capacity)):
            first = x * capacity + at
            fixed, scale = encode(sums[first : first + size, :])
            send[x, at : at + size, :] = fixed
            tally[x, group + p : group + p + 1, :] = scale
    each, key_rows, height = cfg["heavy_each"], cfg["key_rows"], cfg["height"]
    small[...] = jnp.zeros(small.shape, F32)
    for d in range(cfg["devices"]):
        small[d * height : d * height + each, :] = heavy_sum[d * each : (d + 1) * each]
        top = (d + 1) * height
        small[top - key_rows : top, :] = hist_key[d * key_rows : (d + 1) * key_rows]


def place_rows(cfg, got, got_tally, key_slot, send, scales, tally, spread, ranks):
    gx, gy, own, kpp = cfg["gx"], cfg["gy"], cfg["own"], cfg["kpp"]
    key_rows, capacity = cfg["key_rows"], cfg["capacity"]
    group = own // LANES
    base = lax.axis_index("gx") * own
    local = key_slot[...] - base
    mine = (local >= 0) & (local < own)
    rank = jnp.where(mine, group_rank(onehot(mine), key_rows), -1.0).astype(jnp.int32)
    local = local.astype(F32)
    for y in range(gy):
        for x in range(gx):
            first = (x * gy + y) * key_rows
            acc = jnp.zeros((kpp, LANES), F32)
            for j in range(key_rows):
                hit = iota((kpp, LANES), 0) == rank[first + j : first + j + 1]
                acc = acc + jnp.where(hit, local[first + j : first + j + 1], 0.0)
            at = (y * gx + x) * kpp
            spread[at : at + kpp, :] = acc
    counts = jnp.concatenate([got_tally[i, 0:group, :] for i in range(gx)], axis=0)
    present = counts > 0.0
    ranks[...] = jnp.where(present, group_rank(onehot(present), group) + 1.0, 0.0)
    total = counts[0:group]
    for i in range(1, gx):
        total = total + counts[i * group : (i + 1) * group]
    tally[...] = total
    values = []
    for i in range(gx):
        decoded = [
            decode(got[i, at : at + size, :], got_tally[i, group + p : group + p + 1, :])
            for p, (at, size) in enumerate(pieces(capacity))
        ]
        values.append(split(jnp.concatenate(decoded, axis=0)))
    quarter = own // gy
    for q in range(gy):
        at = slice(q * quarter, (q + 1) * quarter)
        slot = jnp.sum(spread[at, :], axis=1, keepdims=True).astype(jnp.int32) - q * quarter
        found = jnp.zeros((quarter, gx), F32)
        for j in range(key_rows):
            hot = onehot(slot - j * LANES == iota((quarter, LANES), 1))
            table = ranks[pl.ds(q * key_rows + j, gx, stride=group), :].astype(BF16)
            found = found + dot(hot, table, NT)
        found = found.astype(jnp.int32) - 1
        out = jnp.zeros((quarter, 2 * LANES), F32)
        for i in range(gx):
            hot = onehot(found[:, i : i + 1] == iota((quarter, capacity), 1))
            out = out + dot(hot, values[i])
        out = out[:, :LANES] + out[:, LANES:]
        for x in range(gx):
            fixed, scale = encode(out[x * kpp : (x + 1) * kpp])
            send[q * gx + x] = fixed
            scales[q * gx + x] = scale


def join_rows(cfg, heavy, got, got_scales, got_small, got_tally, orders, key_slot, result, report, slot_rows, sums, joined):
    gx, gy, own, kpp = cfg["gx"], cfg["gy"], cfg["own"], cfg["kpp"]
    key_rows, height, each = cfg["key_rows"], cfg["height"], cfg["heavy_each"]
    key_dev = key_rows * LANES
    device = lax.axis_index("gx") * gy + lax.axis_index("gy")
    total = got_tally[0:key_rows]
    for y in range(1, gy):
        total = total + got_tally[y * key_rows : (y + 1) * key_rows]
    slot_rows[...] = total
    small = got_small[0:height]
    for d in range(1, cfg["devices"]):
        small = small + got_small[d * height : (d + 1) * height]
    for x in range(gx):
        part = decode(got[x * gy], got_scales[x * gy])
        for y in range(1, gy):
            part = part + decode(got[x * gy + y], got_scales[x * gy + y])
        sums[x * kpp : (x + 1) * kpp, :] = part
    values = split(sums[...])
    owner = key_slot[pl.ds(device * key_rows, key_rows), :] // own
    flags = jnp.concatenate([jnp.where(owner == x, 1.0, 0.0) for x in range(gx)], axis=0)
    rank = group_rank(flags.astype(BF16), key_rows)
    place = jnp.zeros((key_rows, LANES), F32)
    for x in range(gx):
        here = rank[x * key_rows : (x + 1) * key_rows] + float(x * kpp)
        place = place + jnp.where(owner == x, here, 0.0)
    counts = small[height - key_rows : height]
    stacked = jnp.concatenate([place, counts], axis=0)
    columns = stacked.T
    for j in range(key_rows):
        at = slice(j * LANES, (j + 1) * LANES)
        where = columns[:, j : j + 1].astype(jnp.int32)
        hot = onehot(where == iota((LANES, key_dev), 1))
        both = dot(hot, values)
        found = both[:, :LANES] + both[:, LANES:]
        for h in range(each):
            spot = heavy[device * each + h] - device * key_dev - j * LANES
            found = found + jnp.where(iota((LANES, LANES), 0) == spot, small[h : h + 1], 0.0)
        scale = lax.rsqrt(1.0 + columns[:, key_rows + j : key_rows + j + 1])
        value = orders[at, :].astype(F32) * found * scale
        joined[at, :] = value
        result[at, :] = value.astype(BF16)
    lines = [
        joined[pl.ds(heavy[device * each + h] - device * key_dev, 1), :] for h in range(each)
    ]
    report[...] = jnp.concatenate(lines, axis=0).astype(BF16)


def all_barrier(gx, gy, me_x, me_y):
    barrier = pltpu.get_barrier_semaphore()
    device = me_x * gy + me_y
    devices = gx * gy

    @pl.loop(1, devices)
    def _(step):
        other = lax.rem(device + step, devices)
        target = (other // gy, lax.rem(other, gy))
        pl.semaphore_signal(barrier, inc=1, device_id=target, device_id_type=MESH)

    pl.semaphore_wait(barrier, devices - 1)


def exchange(me, count, moves, address):
    for source, landing, send_sem, recv_sem, local_sem in moves:
        pltpu.make_async_copy(source(me), landing(me), local_sem).start()

    def remote(other, move):
        source, landing, send_sem, recv_sem, local_sem = move
        return pltpu.make_async_remote_copy(
            src_ref=source(other),
            dst_ref=landing(me),
            send_sem=send_sem.at[other],
            recv_sem=recv_sem.at[me],
            device_id=address(other),
            device_id_type=MESH,
        )

    def finish(other, move):
        source, landing, send_sem, recv_sem, local_sem = move
        copy = pltpu.make_async_remote_copy(
            src_ref=source(other),
            dst_ref=landing(other),
            send_sem=send_sem.at[other],
            recv_sem=recv_sem.at[other],
            device_id=address(other),
            device_id_type=MESH,
        )
        copy.wait_send()
        copy.wait_recv()

    @pl.loop(1, count)
    def _(step):
        for move in moves:
            remote(lax.rem(me + step, count), move).start()

    def end():
        @pl.loop(1, count)
        def _(step):
            for move in moves:
                finish(lax.rem(me + step, count), move)

        for source, landing, send_sem, recv_sem, local_sem in moves:
            pltpu.make_async_copy(source(me), landing(me), local_sem).wait()

    return end


def to_owners(gx, gy, send, tally, small, got, got_tally, got_small, sem_a, sem_b, sem_c, sem_d, sem_e, sem_f, local):
    me_x, me_y = lax.axis_index("gx"), lax.axis_index("gy")
    all_barrier(gx, gy, me_x, me_y)
    rows = (lambda i: send.at[i], lambda i: got.at[i], sem_a, sem_b, local.at[0])
    tallies = (lambda i: tally.at[i], lambda i: got_tally.at[i], sem_c, sem_d, local.at[1])
    end_x = exchange(me_x, gx, [rows, tallies], lambda i: (i, me_y))
    others = (lambda i: small.at[i], lambda i: got_small.at[i], sem_e, sem_f, local.at[2])
    end_all = exchange(
        me_x * gy + me_y, gx * gy, [others], lambda i: (i // gy, lax.rem(i, gy))
    )
    end_x()
    end_all()


def to_ranges(gx, gy, send, scales, tally, got, got_scales, got_tally, sem_a, sem_b, sem_c, sem_d, sem_e, sem_f, local):
    me_x, me_y = lax.axis_index("gx"), lax.axis_index("gy")
    all_barrier(gx, gy, me_x, me_y)
    rows = (
        lambda i: send.at[lax.rem(i, gy) * gx + i // gy],
        lambda i: got.at[i],
        sem_a,
        sem_b,
        local.at[0],
    )
    factors = (
        lambda i: scales.at[lax.rem(i, gy) * gx + i // gy],
        lambda i: got_scales.at[i],
        sem_e,
        sem_f,
        local.at[2],
    )
    end_all = exchange(
        me_x * gy + me_y, gx * gy, [rows, factors], lambda i: (i // gy, lax.rem(i, gy))
    )
    tallies = (lambda i: tally.at[i], lambda i: got_tally.at[i], sem_c, sem_d, local.at[1])
    end_y = exchange(me_y, gy, [tallies], lambda i: (me_x, i))
    end_y()
    end_all()


def shaped(*dims, dtype=F32):
    return jax.ShapeDtypeStruct(dims, dtype)


def split_body(measures, row_keys, orders, heavy_keys, key_slot):
    rows, columns = measures.shape
    gx, gy = lax.axis_size("gx"), lax.axis_size("gy")
    devices = gx * gy
    key_dev = orders.shape[0]
    key_rows = key_dev // LANES
    own = key_dev * gy
    nr = key_slot.shape[0] // LANES
    heavy = heavy_keys.shape[0]
    each = heavy // devices
    capacity = max(rows // 32, 3 * rows // (4 * gx)) // 4
    segments = gx * capacity
    cfg = dict(
        rows=rows,
        block=min(rows, 2048),
        nr=nr,
        gx=gx,
        gy=gy,
        devices=devices,
        own=own,
        kpp=key_dev // gx,
        key_rows=key_rows,
        heavy=heavy,
        heavy_each=each,
        height=-(-(each + key_rows) // 8) * 8,
        capacity=capacity,
        segments=segments,
        seg_block=512 if segments % 512 == 0 else segments,
    )
    height = cfg["height"]
    group = own // LANES
    params = pltpu.CompilerParams(vmem_limit_bytes=LIMIT)
    table = key_slot.reshape(nr, LANES)
    kpp = cfg["kpp"]
    tall = group + -(-len(pieces(capacity)) // 8) * 8
    send, tally, small = pl.pallas_call(
        functools.partial(gather_rows, cfg),
        out_shape=(
            shaped(gx, capacity, columns, dtype=jnp.int16),
            shaped(gx, tall, LANES),
            shaped(devices * height, LANES),
        ),
        in_specs=[VMEM] * 4,
        out_specs=(VMEM,) * 3,
        scratch_shapes=[pltpu.VMEM((1, rows), jnp.int32), pltpu.VMEM((segments, columns), F32)],
        compiler_params=params,
    )(measures, row_keys.reshape(1, rows), heavy_keys.reshape(heavy, 1), table)
    dma = pltpu.SemaphoreType.DMA
    got, got_tally, got_small = pl.pallas_call(
        functools.partial(to_owners, gx, gy),
        out_shape=(
            shaped(gx, capacity, columns, dtype=jnp.int16),
            shaped(gx, tall, LANES),
            shaped(devices, height, LANES),
        ),
        in_specs=[ANY] * 3,
        out_specs=(ANY,) * 3,
        scratch_shapes=[dma((gx,))] * 4 + [dma((devices,))] * 2 + [dma((3,))],
        compiler_params=pltpu.CompilerParams(collective_id=0, has_side_effects=True),
    )(send, tally, small.reshape(devices, height, LANES))
    send2, scales2, tally2 = pl.pallas_call(
        functools.partial(place_rows, cfg),
        out_shape=(
            shaped(devices, kpp, columns, dtype=jnp.int16),
            shaped(devices, 1, LANES),
            shaped(group, LANES),
        ),
        in_specs=[VMEM] * 3,
        out_specs=(VMEM,) * 3,
        scratch_shapes=[pltpu.VMEM((own, LANES), F32), pltpu.VMEM((gx * group, LANES), F32)],
        compiler_params=params,
    )(got, got_tally, table)
    got2, got_scales2, got_tally2 = pl.pallas_call(
        functools.partial(to_ranges, gx, gy),
        out_shape=(
            shaped(devices, kpp, columns, dtype=jnp.int16),
            shaped(devices, 1, LANES),
            shaped(gy, key_rows, LANES),
        ),
        in_specs=[ANY] * 3,
        out_specs=(ANY,) * 3,
        scratch_shapes=[dma((devices,))] * 2
        + [dma((gy,))] * 2
        + [dma((devices,))] * 2
        + [dma((3,))],
        compiler_params=pltpu.CompilerParams(collective_id=1, has_side_effects=True),
    )(send2, scales2, tally2.reshape(gy, key_rows, LANES))
    result, report, slot_rows = pl.pallas_call(
        functools.partial(join_rows, cfg),
        out_shape=(
            shaped(key_dev, columns, dtype=BF16),
            shaped(each, columns, dtype=BF16),
            shaped(key_rows, LANES),
        ),
        in_specs=[SMEM] + [VMEM] * 6,
        out_specs=(VMEM,) * 3,
        scratch_shapes=[pltpu.VMEM((key_dev, LANES), F32)] * 2,
        compiler_params=params,
    )(
        heavy_keys,
        got2,
        got_scales2,
        got_small.reshape(devices * height, LANES),
        got_tally2.reshape(gy * key_rows, LANES),
        orders,
        table,
    )
    return (result, report, slot_rows.reshape(key_dev))


def fused(
    cfg, measures, keys_hbm, heavy_hbm, table_hbm,
    got2, scales2, hgot, side_out,
    keys, heavy, table, side, rows_in, pair, parity, seg_hot, group_row, local_row, hist, hist16, send1, got1, goth, cnt_got,
    codes, ranks, found, wide, hsend, send2, srow, tsend, tgot,
    load_sem, in_sem, out_sem, back_sem, row_sem, own_sem,
):
    gx, gy, nr, rows, block = cfg["gx"], cfg["gy"], cfg["nr"], cfg["rows"], cfg["block"]
    devices, own, kpp, key_rows = cfg["devices"], cfg["own"], cfg["kpp"], cfg["key_rows"]
    cap, extra, seg, deep = cfg["cap"], cfg["extra"], cfg["seg"], cfg["deep"]
    each, planes, half_seg = cfg["each"], cfg["planes"], cfg["seg"] // 2
    used, at_once = (cap + extra) // 2, cfg["at_once"]
    key_dev = key_rows * LANES
    per_tile = LANES // kpp
    mx, my = lax.axis_index("gx"), lax.axis_index("gy")
    me = mx * gy + my
    z, j = me // gx, lax.rem(me, gx)

    def remote(src, dst, send_sem, recv_sem, where):
        return pltpu.make_async_remote_copy(
            src_ref=src, dst_ref=dst, send_sem=send_sem, recv_sem=recv_sem,
            device_id=where, device_id_type=MESH,
        )

    def in_plane(p, x):
        d = p * gx + x
        return (d // gy, lax.rem(d, gy))

    beside = [lax.rem(my + s, gy) for s in range(gy)]

    def every_other(act):
        for y in beside[1:]:
            act(mx * gy + y, (mx, y))

        @pl.loop(1, gx)
        def _(s):
            x = lax.rem(mx + s, gx)
            for y in beside:
                act(x * gy + y, (x, y))

    self_id = (mx, my)
    others = devices - 1
    COUNTS, HISTS, ROWS, MERGED, SCALES, HEADS, TOTALS = range(7)

    loads = [
        pltpu.make_async_copy(source, target, in_sem.at[i])
        for i, (source, target) in enumerate(
            [(keys_hbm, keys), (heavy_hbm, heavy), (table_hbm, table)]
        )
    ]
    for one in loads:
        one.start()
    load = pltpu.make_async_copy(measures, rows_in, load_sem)
    load.start()

    steps_to = sorted(range(1, gx), key=lambda m: (-bin(m >> 1).count("1"), m & 1, -m)) + [0]
    partner = []
    for m in steps_to:
        x, bit = j, 1
        while bit < gx:
            if m & bit:
                x = x + bit * (1 - 2 * lax.rem(x // bit, 2))
            bit *= 2
        partner.append(x)

    barrier = pltpu.get_barrier_semaphore()

    every_other(
        lambda d, where: pl.semaphore_signal(
            barrier, inc=1, device_id=where, device_id_type=MESH
        )
    )
    for one in loads:
        one.wait()

    chains = [jnp.zeros((nr, LANES), F32)] * 2
    for c in range(rows // block):
        span = slice(c * block, (c + 1) * block)
        key = keys[:, span]
        row_hot = onehot(iota((nr, block), 0) == key >> 7)
        seg_hot[:, span] = row_hot
        column_hot = onehot(iota((LANES, block), 0) == (key & 127))
        chains[c % 2] = chains[c % 2] + dot(row_hot, column_hot, NT)
    total = joined_chains(chains)
    hist[...] = total.reshape(devices, key_rows, LANES)
    hist16[...] = total.astype(jnp.int32).astype(jnp.int16)
    cnt_got[me] = hist[me]

    owner = table[...] // own
    heavy_key = heavy[...]
    heads = heavy_key.shape[1]
    code = iota((1, heads), 1) + 1
    row_of = iota((nr, heads), 0) == heavy_key >> 7
    col_of = onehot(iota((LANES, heads), 0) == (heavy_key & 127))
    low = dot(jnp.where(row_of, (code & 127).astype(F32), 0.0).astype(BF16), col_of, NT)
    high = dot(jnp.where(row_of, (code >> 7).astype(F32), 0.0).astype(BF16), col_of, NT)
    which = (low + 128.0 * high).astype(jnp.int32)
    codes[...] = which.astype(F32).reshape(devices, key_rows, LANES)
    light = which == 0
    present = (total > 0.0) & light
    lane_r, lane_c = iota((LANES, 2 * LANES), 0), iota((LANES, 2 * LANES), 1)
    upper = onehot((lane_c >= LANES) | (lane_r < lane_c))
    lower = onehot(iota((nr, nr), 1) < iota((nr, nr), 0))
    flags = jnp.concatenate(
        [jnp.where(present & (owner == x), 1.0, 0.0) for x in range(gx)], axis=0
    ).astype(BF16)
    both = dot(flags, upper)
    local = jnp.zeros((nr, LANES), F32)
    for x in range(gx):
        part = both[x * nr : (x + 1) * nr]
        rank = part[:, :LANES] + dot(lower, part[:, LANES:].astype(BF16))
        local = local + jnp.where(owner == x, rank, 0.0)
    head = which - 1
    block_of = head // each
    group = jnp.where(light, owner, lax.rem(block_of, gx))
    local = jnp.where(
        light, local, (cap + (block_of // gx) * each + lax.rem(head, each)).astype(F32)
    )
    tables = jnp.concatenate([256.0 * group.astype(F32).T, local.T], axis=1).astype(BF16)
    pl.semaphore_wait(barrier, devices - 1)

    for s in range(gx - 1):
        remote(
            hist16, goth.at[s], out_sem.at[HISTS], back_sem.at[HISTS], in_plane(z, partner[s])
        ).start()
    every_other(
        lambda d, where: remote(
            hist.at[d], cnt_got.at[me], out_sem.at[COUNTS], back_sem.at[COUNTS], where
        ).start()
    )

    load.wait()
    for c in range(rows // block):
        span = slice(c * block, (c + 1) * block)
        row_hot = seg_hot[:, span]
        spread = dot(tables, jnp.concatenate([row_hot, row_hot], axis=0))
        mask = iota((LANES, block), 0) == (keys[:, span] & 127)
        both = jnp.sum(jnp.where(mask, spread, 0.0), axis=0, keepdims=True).astype(jnp.int32)
        group_row[:, span] = both >> 8
        inside = both & 255
        local_row[:, span] = inside >> 1
        odd = (inside & 1).astype(F32)
        for i in range(block // LANES):
            at = c * (block // LANES) + i
            parity[at : at + 1, :] = odd[:, i * LANES : (i + 1) * LANES]

    turned = parity[...].T
    for c in range(rows // LANES):
        span = slice(c * LANES, (c + 1) * LANES)
        line = rows_in[span, :]
        odd = line * jnp.broadcast_to(turned[:, c : c + 1], (LANES, LANES)).astype(BF16)
        pair[span, LANES:] = odd
        pair[span, :LANES] = line - odd

    def encode(values):
        largest = jnp.max(jnp.abs(values), axis=1, keepdims=True)
        power = jnp.floor(jnp.log2(jnp.maximum(largest, 1e-30))) + 1.0
        fixed = jnp.clip(jnp.round(values * jnp.exp2(15.0 - power)), -32767.0, 32767.0)
        return fixed, power

    for first in range(0, gx, at_once):
        steps = range(first, first + at_once)
        chains = [jnp.zeros((at_once * half_seg, 2 * LANES), F32)] * 2
        for c in range(rows // block):
            span = slice(c * block, (c + 1) * block)
            group, local = group_row[:, span], local_row[:, span]
            hot = [
                jnp.where(
                    iota((half_seg, block), 0)
                    == jnp.where(group == partner[s], local, -1),
                    1.0,
                    0.0,
                )
                for s in steps
            ]
            chains[c % 2] = chains[c % 2] + dot(
                jnp.concatenate(hot, axis=0).astype(BF16), pair[span, :]
            )
        acc = joined_chains(chains)
        for s in steps:
            at = (s - first) * half_seg
            both = acc[at : at + half_seg]
            fixed, power = encode(jnp.concatenate([both[:, :LANES], both[:, LANES:]], axis=0))
            lines = []
            for top, size in pieces(seg):
                diagonal = iota((size, LANES), 0) == iota((size, LANES), 1)
                lines.append(
                    jnp.sum(jnp.where(diagonal, power[top : top + size], 0.0), axis=0, keepdims=True)
                )
            foot = jnp.zeros((half_seg - used, LANES), F32)
            for n, one in enumerate(lines):
                foot = jnp.where(iota(foot.shape, 0) == n, one, foot)
            whole = jnp.concatenate([fixed[:used], foot, fixed[half_seg:]], axis=0)
            send1[s] = whole.astype(jnp.int32).astype(jnp.int16)
            if s < gx - 1:
                remote(
                    send1.at[s], got1.at[s], out_sem.at[ROWS], row_sem.at[s],
                    in_plane(z, partner[s]),
                ).start()

    def all_of(ref, kind, number):
        return remote(
            ref.at[0:number], ref.at[0:number], out_sem.at[kind], back_sem.at[kind], self_id
        )

    all_of(goth, HISTS, gx - 1).wait_recv()
    mine = (owner == j) & light
    arrived = []
    for t in range(gx):
        here = hist16[...] if t == gx - 1 else goth[t]
        arrived.append(jnp.where((here.astype(jnp.int32) > 0) & mine, 1.0, 0.0))
    flags = jnp.concatenate(arrived, axis=0)
    both = dot(flags.astype(BF16), upper)
    for t in range(gx):
        part = both[t * nr : (t + 1) * nr]
        rank = (part[:, :LANES] + dot(lower, part[:, LANES:].astype(BF16))).astype(jnp.int32)
        rank = ((rank >> 1) + (rank & 1) * half_seg + 1).astype(F32)
        ranks[t * nr : (t + 1) * nr, :] = rank * flags[t * nr : (t + 1) * nr]
    own_flags = onehot(owner == j)
    both = dot(own_flags, upper)
    row_r, row_c = iota((nr, nr), 0), iota((nr, nr), 1)
    near = onehot((row_c < row_r) & (row_r // key_rows == row_c // key_rows))
    rank = both[:, :LANES] + dot(near, both[:, LANES:].astype(BF16))
    rank = jnp.where(owner == j, rank, -1.0).astype(jnp.int32)
    for d in range(devices):
        hot, tall = [], []
        for q in range(key_rows):
            r = d * key_rows + q
            hot.append(onehot(iota((kpp, LANES), 0) == rank[r : r + 1]))
            tall.append(ranks[pl.ds(r, gx, stride=nr), :].astype(BF16))
        found[d * kpp : (d + 1) * kpp, 0:gx] = dot(
            jnp.concatenate(hot, axis=1), jnp.concatenate(tall, axis=1), NT
        )

    all_of(cnt_got, COUNTS, others).wait()

    counted = cnt_got[0]
    for d in range(1, devices):
        counted = counted + cnt_got[d]
    side[key_rows : 2 * key_rows, :] = counted
    tsend[...] = jnp.where(codes[me] == 0.0, counted, 0.0)
    tgot[mx] = tsend[...]

    @pl.loop(1, gx)
    def _(s):
        x = lax.rem(mx + s, gx)
        remote(tsend, tgot.at[mx], out_sem.at[TOTALS], back_sem.at[TOTALS], (x, my)).start()

    heads_sum = [jnp.zeros((extra // 2, LANES), F32)] * 2
    powers = []
    for t in range(gx):
        if t < gx - 1:
            remote(send1.at[t], got1.at[t], out_sem.at[ROWS], row_sem.at[t], self_id).wait_recv()
            block16 = got1[t]
        else:
            block16 = send1[t]
        value = block16.astype(jnp.int32)
        wide[t, 0:seg, :LANES] = (value >> 8).astype(F32).astype(BF16)
        wide[t, 0:seg, LANES:] = (value & 255).astype(F32).astype(BF16)
        if deep > seg:
            wide[t, seg:deep, :] = jnp.zeros((deep - seg, 2 * LANES), BF16)
        scale = jnp.exp2(value[used : used + len(pieces(seg))].astype(F32) - 15.0)
        powers.append(
            jnp.concatenate([scale[p : p + 1] for p in range(deep // LANES)], axis=1)
        )
        for b in range(2):
            top = b * half_seg + cap // 2
            p, at = top // LANES, top % LANES
            column = jnp.sum(
                jnp.where(
                    iota((extra // 2, LANES), 1) == iota((extra // 2, LANES), 0) + at,
                    scale[p : p + 1],
                    0.0,
                ),
                axis=1, keepdims=True,
            )
            heads_sum[b] = heads_sum[b] + value[top : top + extra // 2].astype(F32) * column
    hsend[...] = jnp.concatenate(heads_sum, axis=0)

    local_heads = pltpu.make_async_copy(hsend, hgot.at[z], own_sem.at[0])
    local_heads.start()

    @pl.loop(1, planes)
    def _(s):
        other = lax.rem(z + s, planes)
        remote(
            hsend, hgot.at[z], out_sem.at[HEADS], back_sem.at[HEADS], in_plane(other, j)
        ).start()

    chunk = gx * kpp
    shift = lax.rem(j, per_tile) * kpp
    half = planes // 2
    lanes = (iota((1, deep), 1) + 1).astype(F32)
    if planes == 4:
        order = [
            lax.rem(z + half, planes), planes - 1 - z,
            planes - 1 - lax.rem(z + half, planes), z,
        ]
    else:
        order = [lax.rem(z + s, planes) for s in range(1, planes + 1)]
    diagonal = iota((kpp, LANES), 1) == iota((kpp, LANES), 0) + shift
    wave = gx // 2
    part = wave * kpp
    for c in range(planes):
        far, last = order[c], c == planes - 1
        for first in range(0, gx, wave):
            top = pl.multiple_of(far * chunk + first * kpp, part)
            spot = found[pl.ds(top, part), :]
            chains = [jnp.zeros((part, 2 * LANES), F32)] * 2
            for t in range(gx):
                hit = spot[:, t : t + 1] == lanes
                chains[t % 2] = chains[t % 2] + dot(
                    jnp.where(hit, powers[t], 0.0).astype(BF16), wide[t]
                )
            acc = joined_chains(chains)
            fixed, power = encode(acc[:, :LANES] * 256.0 + acc[:, LANES:])
            send2[c, first : first + wave] = (
                fixed.astype(jnp.int32).astype(jnp.int16).reshape(wave, kpp, LANES)
            )
            scale = jnp.exp2(power - 15.0)
            for x in range(wave):
                srow[c, first + x] = jnp.sum(
                    jnp.where(diagonal, scale[x * kpp : (x + 1) * kpp], 0.0), axis=0, keepdims=True
                )

            def one_block(x, c=c, far=far):
                where = in_plane(far, x)
                remote(
                    send2.at[c, x], got2.at[me], out_sem.at[MERGED], back_sem.at[MERGED], where
                ).start()
                remote(
                    srow.at[c, x], scales2.at[me], out_sem.at[SCALES], back_sem.at[SCALES], where
                ).start()

            @pl.loop(0, wave)
            def _(s, first=first, last=last, one_block=one_block):
                x = first + lax.rem(j + s, wave)
                if last:
                    pl.when(x != j)(lambda: one_block(x))
                else:
                    one_block(x)

    keep = pltpu.make_async_copy(send2.at[planes - 1, j], got2.at[me], own_sem.at[1])
    keep.start()
    keep_row = pltpu.make_async_copy(srow.at[planes - 1, j], scales2.at[me], own_sem.at[2])
    keep_row.start()

    all_of(tgot, TOTALS, gx - 1).wait()

    base = me * key_dev
    left, right = [], []
    for m in range(gx):
        slots = table[pl.ds((m * gy + my) * key_rows, key_rows), :] - base
        for q in range(key_rows):
            line = slots[q : q + 1]
            amount = tgot[m, q : q + 1, :].astype(jnp.int32)
            bands = [
                jnp.where(
                    iota((8, LANES), 0) == (line >> 7), ((amount >> (8 * b)) & 255).astype(F32), 0.0
                )
                for b in range(3)
            ]
            left.append(jnp.concatenate(bands + [jnp.zeros((8, LANES), F32)], axis=0).astype(BF16))
            right.append(onehot(iota((LANES, LANES), 0) == (line & 127)))
    middle = len(left) // 2
    bands = joined_chains(
        [
            dot(jnp.concatenate(left[part], axis=1), jnp.concatenate(right[part], axis=1), NT)
            for part in (slice(0, middle), slice(middle, None))
        ]
    )
    side[2 * key_rows : 3 * key_rows, :] = (
        bands[0:8] + 256.0 * bands[8:16] + 65536.0 * bands[16:24]
    )[0:key_rows]
    owner = table[pl.ds(me * key_rows, key_rows), :] // own
    flags = jnp.concatenate([jnp.where(owner == x, 1.0, 0.0) for x in range(gx)], axis=0)
    rank = group_rank(flags.astype(BF16), key_rows)
    place = jnp.zeros((key_rows, LANES), F32)
    for x in range(gx):
        inside = rank[x * key_rows : (x + 1) * key_rows] + float(x * kpp)
        place = place + jnp.where(owner == x, inside, 0.0)
    side[0:key_rows, :] = place
    side[3 * key_rows : 4 * key_rows, :] = codes[me] - (each * me).astype(F32)
    hand_over = pltpu.make_async_copy(side, side_out, own_sem.at[3])
    hand_over.start()

    all_of(goth, HISTS, gx - 1).wait_send()
    all_of(send1, ROWS, gx - 1).wait_send()
    local_heads.wait()
    keep.wait()
    keep_row.wait()
    hand_over.wait()
    all_of(hgot, HEADS, planes - 1).wait()
    all_of(got2, MERGED, others).wait()
    all_of(scales2, SCALES, others).wait()


def join(
    cfg, got_hbm, scales_hbm, heads_hbm, side_hbm, orders_hbm, result, report, slot_rows,
    got, scales, heads, side, orders, done, lines_out, sems, out_sems,
):
    gx, gy, kpp = cfg["gx"], cfg["gy"], cfg["kpp"]
    key_rows, each, planes, extra = cfg["key_rows"], cfg["each"], cfg["planes"], cfg["extra"]
    key_dev = key_rows * LANES
    per_tile = LANES // kpp
    loads = [
        pltpu.make_async_copy(got_hbm.at[p * gx : (p + 1) * gx], got.at[p], sems.at[4 + p])
        for p in range(planes)
    ]
    tables = [
        pltpu.make_async_copy(source, target, sems.at[i])
        for i, (source, target) in enumerate(
            [(side_hbm, side), (scales_hbm, scales), (heads_hbm, heads), (orders_hbm, orders)]
        )
    ]
    for one in tables[:2] + loads + tables[2:]:
        one.start()
    z = (lax.axis_index("gx") * gy + lax.axis_index("gy")) // gx
    tables[0].wait()
    tables[1].wait()
    columns = side[...].T
    stores = [
        pltpu.make_async_copy(
            side.at[2 * key_rows : 3 * key_rows, :], slot_rows, out_sems.at[key_rows]
        )
    ]
    stores[0].start()
    lines = []
    for p in range(planes):
        tiles = []
        for x in range(0, gx, per_tile):
            tile = scales[p * gx + x]
            for i in range(1, per_tile):
                tile = tile + scales[p * gx + x + i]
            tiles.append(tile)
        lines.append(jnp.concatenate(tiles, axis=1))
    tables[2].wait()
    tables[3].wait()
    small = heads[0]
    for p in range(1, planes):
        small = small + heads[p]
    own_lines = []
    for h in range(each):
        entry = z * each + h
        spot = lax.rem(entry, 2) * (extra // 2) + entry // 2
        own_lines.append(
            jnp.sum(jnp.where(iota((extra, LANES), 0) == spot, small, 0.0), axis=0, keepdims=True)
        )
    values = []
    for p in range(planes):
        loads[p].wait()
        value = got[p].reshape(key_dev, LANES).astype(jnp.int32)
        values.append(
            jnp.concatenate([(value >> 8).astype(F32), (value & 255).astype(F32)], axis=1).astype(BF16)
        )
    picked = [jnp.zeros((1, LANES), F32)] * each
    for q in range(key_rows):
        at = slice(q * LANES, (q + 1) * LANES)
        hit = columns[:, q : q + 1] == iota((LANES, key_dev), 1).astype(F32)
        chains = [jnp.zeros((LANES, 2 * LANES), F32)] * 2
        for p in range(planes):
            chains[p % 2] = chains[p % 2] + dot(
                jnp.where(hit, lines[p], 0.0).astype(BF16), values[p]
            )
        both = joined_chains(chains)
        sums = both[:, :LANES] * 256.0 + both[:, LANES:]
        head = columns[:, 3 * key_rows + q : 3 * key_rows + q + 1]
        for h in range(each):
            sums = sums + jnp.where(head == float(h + 1), own_lines[h], 0.0)
        scale = lax.rsqrt(1.0 + columns[:, key_rows + q : key_rows + q + 1])
        value = orders[at, :].astype(F32) * sums * scale
        for h in range(each):
            picked[h] = picked[h] + jnp.sum(
                jnp.where(head == float(h + 1), value, 0.0), axis=0, keepdims=True
            )
        done[at, :] = value.astype(BF16)
        stores.append(pltpu.make_async_copy(done.at[at, :], result.at[at, :], out_sems.at[q]))
        stores[-1].start()
    lines_out[...] = jnp.concatenate(picked, axis=0).astype(BF16)
    stores.append(pltpu.make_async_copy(lines_out, report, out_sems.at[key_rows + 1]))
    stores[-1].start()
    for one in stores:
        one.wait()


def body(measures, row_keys, orders, heavy_keys, key_slot):
    rows, columns = measures.shape
    gx, gy = lax.axis_size("gx"), lax.axis_size("gy")
    devices = gx * gy
    key_dev = orders.shape[0]
    key_rows = key_dev // LANES
    nr = key_slot.shape[0] // LANES
    heavy = heavy_keys.shape[0]
    each = heavy // devices
    if gx * nr > 2048 or gx & (gx - 1):
        return split_body(measures, row_keys, orders, heavy_keys, key_slot)
    planes = devices // gx
    cap = max(rows // 32, 3 * rows // (4 * gx)) // 4
    extra = planes * each
    seg = 2 * (-(-((cap + extra) // 2 + len(pieces(cap + extra + 16))) // 8) * 8)
    deep = -(-cap // LANES) * LANES
    kpp = key_dev // gx
    cfg = dict(
        rows=rows, block=min(rows, 2048), nr=nr, gx=gx, gy=gy, devices=devices,
        own=key_dev * gy, kpp=kpp, key_rows=key_rows, each=each, planes=planes,
        cap=cap, extra=extra, seg=seg, at_once=2 if gx % 2 == 0 else gx, deep=max(deep, -(-seg // LANES) * LANES),
    )
    deep = cfg["deep"]
    table = key_slot.reshape(nr, LANES)
    dma = pltpu.SemaphoreType.DMA
    i16 = jnp.int16
    got, scales, heads, side = pl.pallas_call(
        functools.partial(fused, cfg),
        out_shape=(
            shaped(devices, kpp, columns, dtype=i16),
            shaped(devices, 1, LANES),
            shaped(planes, extra, LANES),
            shaped(4 * key_rows, LANES),
        ),
        in_specs=[ANY] * 4,
        out_specs=(ANY,) * 4,
        scratch_shapes=[
            pltpu.VMEM((1, rows), jnp.int32),
            pltpu.VMEM((1, heavy), jnp.int32),
            pltpu.VMEM((nr, LANES), jnp.int32),
            pltpu.VMEM((4 * key_rows, LANES), F32),
            pltpu.VMEM((rows, columns), BF16),
            pltpu.VMEM((rows, 2 * columns), BF16),
            pltpu.VMEM((rows // LANES, LANES), F32),
            pltpu.VMEM((nr, rows), BF16),
            pltpu.VMEM((1, rows), jnp.int32),
            pltpu.VMEM((1, rows), jnp.int32),
            pltpu.VMEM((devices, key_rows, LANES), F32),
            pltpu.VMEM((nr, LANES), i16),
            pltpu.VMEM((gx, seg, LANES), i16),
            pltpu.VMEM((gx, seg, LANES), i16),
            pltpu.VMEM((gx, nr, LANES), i16),
            pltpu.VMEM((devices, key_rows, LANES), F32),
            pltpu.VMEM((devices, key_rows, LANES), F32),
            pltpu.VMEM((gx * nr, LANES), F32),
            pltpu.VMEM((devices * kpp, LANES), F32),
            pltpu.VMEM((gx, deep, 2 * LANES), BF16),
            pltpu.VMEM((extra, LANES), F32),
            pltpu.VMEM((planes, gx, kpp, LANES), i16),
            pltpu.VMEM((planes, gx, 1, LANES), F32),
            pltpu.VMEM((key_rows, LANES), F32),
            pltpu.VMEM((gx, key_rows, LANES), F32),
            dma,
            dma((3,)),
            dma((7,)),
            dma((7,)),
            dma((gx,)),
            dma((4,)),
        ],
        compiler_params=pltpu.CompilerParams(
            collective_id=2, has_side_effects=True, vmem_limit_bytes=LIMIT
        ),
    )(measures, row_keys.reshape(1, rows), heavy_keys.reshape(1, heavy), table)
    result, report, slot_rows = pl.pallas_call(
        functools.partial(join, cfg),
        out_shape=(
            shaped(key_dev, columns, dtype=BF16),
            shaped(each, columns, dtype=BF16),
            shaped(key_rows, LANES),
        ),
        in_specs=[ANY] * 5,
        out_specs=(ANY,) * 3,
        scratch_shapes=[
            pltpu.VMEM((planes, gx, kpp, columns), i16),
            pltpu.VMEM((devices, 1, LANES), F32),
            pltpu.VMEM((planes, extra, LANES), F32),
            pltpu.VMEM((4 * key_rows, LANES), F32),
            pltpu.VMEM((key_dev, columns), BF16),
            pltpu.VMEM((key_dev, columns), BF16),
            pltpu.VMEM((each, columns), BF16),
            dma((4 + planes,)),
            dma((key_rows + 2,)),
        ],
        compiler_params=pltpu.CompilerParams(vmem_limit_bytes=LIMIT),
    )(got, scales, heads, side, orders)
    return (result, report, slot_rows.reshape(key_dev))


def solution(mesh):
    return jax.shard_map(
        body,
        mesh=mesh,
        in_specs=(P(("gx", "gy"), None), P(("gx", "gy")), P(("gx", "gy"), None), P(), P()),
        out_specs=(P(("gx", "gy"), None), P(("gx", "gy"), None), P(("gx", "gy"))),
        check_vma=False,
    )
```

```python
import functools

import jax
import jax.numpy as jnp
from jax import lax
from jax.experimental import pallas as pl
from jax.experimental.pallas import tpu as pltpu
from jax.sharding import PartitionSpec as P

MESH = pl.DeviceIdType.MESH
LANES = 128
LEAST = -3.4028235e38
F32 = jnp.float32
BF16 = jnp.bfloat16
VMEM = pl.BlockSpec(memory_space=pltpu.VMEM)
ANY = pl.BlockSpec(memory_space=pl.ANY)
SMEM = pl.BlockSpec(memory_space=pltpu.SMEM)
LIMIT = 60 * 1024 * 1024
NN = (((1,), (0,)), ((), ()))
NT = (((1,), (1,)), ((), ()))


def dot(a, b, dims=NN):
    return lax.dot_general(a, b, dims, preferred_element_type=F32)


def iota(shape, dim):
    return lax.broadcasted_iota(jnp.int32, shape, dim)


def onehot(mask):
    return jnp.where(mask, 1.0, 0.0).astype(BF16)


def group_rank(flags, group_rows):
    rows = flags.shape[0]
    lane_r, lane_c = iota((LANES, LANES), 0), iota((LANES, LANES), 1)
    inside = dot(flags, onehot(lane_r < lane_c))
    whole = dot(flags, onehot(lane_r >= 0))
    row_r, row_c = iota((rows, rows), 0), iota((rows, rows), 1)
    earlier = onehot((row_c < row_r) & (row_r // group_rows == row_c // group_rows))
    return inside + dot(earlier, whole.astype(BF16))


def split(values):
    high = values.astype(BF16)
    low = (values - high.astype(F32)).astype(BF16)
    return jnp.concatenate([high, low], axis=1)


def eye(rows):
    return iota((rows, LANES), 0) == iota((rows, LANES), 1)


def encode(values):
    largest = jnp.max(jnp.abs(values), axis=1, keepdims=True)
    safe = jnp.maximum(largest, 1e-30)
    fixed = jnp.round(values * (1.0 / safe) * 32767.0).astype(jnp.int32).astype(jnp.int16)
    return fixed, jnp.sum(jnp.where(eye(values.shape[0]), safe, 0.0), axis=0, keepdims=True)


def decode(fixed, scale):
    column = jnp.sum(jnp.where(eye(fixed.shape[0]), scale, 0.0), axis=1, keepdims=True)
    return fixed.astype(jnp.int32).astype(F32) * (column * (1.0 / 32767.0))


def joined_chains(chains):
    return chains[0] + jnp.maximum(chains[1], LEAST)


def pieces(total):
    return [(at, min(LANES, total - at)) for at in range(0, total, LANES)]


def byte_table(table, parts):
    pieces = [((table >> (8 * p)) & 255).astype(F32).T for p in range(parts)]
    return jnp.concatenate(pieces, axis=0).astype(BF16)


def look_up(bytes_table, row_hot, column_mask, parts):
    wide = dot(bytes_table, row_hot)
    found = 0.0
    for p in range(parts):
        piece = wide[p * LANES : (p + 1) * LANES]
        found = found + float(256**p) * jnp.sum(
            jnp.where(column_mask, piece, 0.0), axis=0, keepdims=True
        )
    return found.astype(jnp.int32)


def byte_count(largest):
    return (int(largest).bit_length() + 7) // 8


def gather_rows(cfg, measures, keys, heavy, key_slot, send, tally, small, slots, sums):
    rows, block, nr = cfg["rows"], cfg["block"], cfg["nr"]
    segments, capacity = cfg["segments"], cfg["capacity"]
    slot_parts = byte_count(nr * LANES - 1)
    slot_bytes = byte_table(key_slot[...], slot_parts)
    hist_key = jnp.zeros((nr, LANES), F32)
    hist_slot = jnp.zeros((nr, LANES), F32)
    heavy_sum = jnp.zeros((cfg["heavy"], LANES), F32)
    for c in range(rows // block):
        span = slice(c * block, (c + 1) * block)
        key = keys[:, span]
        row_hot = onehot(iota((nr, block), 0) == key >> 7)
        column_mask = iota((LANES, block), 0) == (key & 127)
        hist_key = hist_key + dot(row_hot, onehot(column_mask), NT)
        heavy_hot = jnp.where(heavy[...] == key, 1.0, 0.0)
        is_heavy = jnp.max(heavy_hot, axis=0, keepdims=True) > 0.0
        heavy_sum = heavy_sum + dot(heavy_hot.astype(BF16), measures[span, :])
        slot = jnp.where(is_heavy, -1, look_up(slot_bytes, row_hot, column_mask, slot_parts))
        slots[:, span] = slot
        slot_row = onehot(iota((nr, block), 0) == slot >> 7)
        slot_column = onehot(iota((LANES, block), 0) == (slot & 127))
        hist_slot = hist_slot + dot(slot_row, slot_column, NT)
    present = hist_slot > 0.0
    group = cfg["own"] // LANES
    tally[...] = jnp.zeros(tally.shape, F32)
    for x in range(cfg["gx"]):
        tally[x, 0:group, :] = hist_slot[x * group : (x + 1) * group]
    rank = group_rank(onehot(present), group).astype(jnp.int32)
    owner = iota((nr, LANES), 0) // group
    segment_table = jnp.where(present, owner * capacity + rank + 1, 0)
    seg_parts = byte_count(segments)
    segment_bytes = byte_table(segment_table, seg_parts)
    step = cfg["seg_block"]
    for c in range(rows // block):
        span = slice(c * block, (c + 1) * block)
        slot = slots[:, span]
        slot_row = onehot(iota((nr, block), 0) == slot >> 7)
        slot_mask = iota((LANES, block), 0) == (slot & 127)
        segment = look_up(segment_bytes, slot_row, slot_mask, seg_parts) - 1
        for s in range(segments // step):
            hot = onehot(iota((step, block), 0) == segment - s * step)
            product = dot(hot, measures[span, :])
            place = slice(s * step, (s + 1) * step)
            if c == 0:
                sums[place, :] = product
            else:
                sums[place, :] += product
    for x in range(cfg["gx"]):
        for p, (at, size) in enumerate(pieces(capacity)):
            first = x * capacity + at
            fixed, scale = encode(sums[first : first + size, :])
            send[x, at : at + size, :] = fixed
            tally[x, group + p : group + p + 1, :] = scale
    each, key_rows, height = cfg["heavy_each"], cfg["key_rows"], cfg["height"]
    small[...] = jnp.zeros(small.shape, F32)
    for d in range(cfg["devices"]):
        small[d * height : d * height + each, :] = heavy_sum[d * each : (d + 1) * each]
        top = (d + 1) * height
        small[top - key_rows : top, :] = hist_key[d * key_rows : (d + 1) * key_rows]


def place_rows(cfg, got, got_tally, key_slot, send, scales, tally, spread, ranks):
    gx, gy, own, kpp = cfg["gx"], cfg["gy"], cfg["own"], cfg["kpp"]
    key_rows, capacity = cfg["key_rows"], cfg["capacity"]
    group = own // LANES
    base = lax.axis_index("gx") * own
    local = key_slot[...] - base
    mine = (local >= 0) & (local < own)
    rank = jnp.where(mine, group_rank(onehot(mine), key_rows), -1.0).astype(jnp.int32)
    local = local.astype(F32)
    for y in range(gy):
        for x in range(gx):
            first = (x * gy + y) * key_rows
            acc = jnp.zeros((kpp, LANES), F32)
            for j in range(key_rows):
                hit = iota((kpp, LANES), 0) == rank[first + j : first + j + 1]
                acc = acc + jnp.where(hit, local[first + j : first + j + 1], 0.0)
            at = (y * gx + x) * kpp
            spread[at : at + kpp, :] = acc
    counts = jnp.concatenate([got_tally[i, 0:group, :] for i in range(gx)], axis=0)
    present = counts > 0.0
    ranks[...] = jnp.where(present, group_rank(onehot(present), group) + 1.0, 0.0)
    total = counts[0:group]
    for i in range(1, gx):
        total = total + counts[i * group : (i + 1) * group]
    tally[...] = total
    values = []
    for i in range(gx):
        decoded = [
            decode(got[i, at : at + size, :], got_tally[i, group + p : group + p + 1, :])
            for p, (at, size) in enumerate(pieces(capacity))
        ]
        values.append(split(jnp.concatenate(decoded, axis=0)))
    quarter = own // gy
    for q in range(gy):
        at = slice(q * quarter, (q + 1) * quarter)
        slot = jnp.sum(spread[at, :], axis=1, keepdims=True).astype(jnp.int32) - q * quarter
        found = jnp.zeros((quarter, gx), F32)
        for j in range(key_rows):
            hot = onehot(slot - j * LANES == iota((quarter, LANES), 1))
            table = ranks[pl.ds(q * key_rows + j, gx, stride=group), :].astype(BF16)
            found = found + dot(hot, table, NT)
        found = found.astype(jnp.int32) - 1
        out = jnp.zeros((quarter, 2 * LANES), F32)
        for i in range(gx):
            hot = onehot(found[:, i : i + 1] == iota((quarter, capacity), 1))
            out = out + dot(hot, values[i])
        out = out[:, :LANES] + out[:, LANES:]
        for x in range(gx):
            fixed, scale = encode(out[x * kpp : (x + 1) * kpp])
            send[q * gx + x] = fixed
            scales[q * gx + x] = scale


def join_rows(cfg, heavy, got, got_scales, got_small, got_tally, orders, key_slot, result, report, slot_rows, sums, joined):
    gx, gy, own, kpp = cfg["gx"], cfg["gy"], cfg["own"], cfg["kpp"]
    key_rows, height, each = cfg["key_rows"], cfg["height"], cfg["heavy_each"]
    key_dev = key_rows * LANES
    device = lax.axis_index("gx") * gy + lax.axis_index("gy")
    total = got_tally[0:key_rows]
    for y in range(1, gy):
        total = total + got_tally[y * key_rows : (y + 1) * key_rows]
    slot_rows[...] = total
    small = got_small[0:height]
    for d in range(1, cfg["devices"]):
        small = small + got_small[d * height : (d + 1) * height]
    for x in range(gx):
        part = decode(got[x * gy], got_scales[x * gy])
        for y in range(1, gy):
            part = part + decode(got[x * gy + y], got_scales[x * gy + y])
        sums[x * kpp : (x + 1) * kpp, :] = part
    values = split(sums[...])
    owner = key_slot[pl.ds(device * key_rows, key_rows), :] // own
    flags = jnp.concatenate([jnp.where(owner == x, 1.0, 0.0) for x in range(gx)], axis=0)
    rank = group_rank(flags.astype(BF16), key_rows)
    place = jnp.zeros((key_rows, LANES), F32)
    for x in range(gx):
        here = rank[x * key_rows : (x + 1) * key_rows] + float(x * kpp)
        place = place + jnp.where(owner == x, here, 0.0)
    counts = small[height - key_rows : height]
    stacked = jnp.concatenate([place, counts], axis=0)
    columns = stacked.T
    for j in range(key_rows):
        at = slice(j * LANES, (j + 1) * LANES)
        where = columns[:, j : j + 1].astype(jnp.int32)
        hot = onehot(where == iota((LANES, key_dev), 1))
        both = dot(hot, values)
        found = both[:, :LANES] + both[:, LANES:]
        for h in range(each):
            spot = heavy[device * each + h] - device * key_dev - j * LANES
            found = found + jnp.where(iota((LANES, LANES), 0) == spot, small[h : h + 1], 0.0)
        scale = lax.rsqrt(1.0 + columns[:, key_rows + j : key_rows + j + 1])
        value = orders[at, :].astype(F32) * found * scale
        joined[at, :] = value
        result[at, :] = value.astype(BF16)
    lines = [
        joined[pl.ds(heavy[device * each + h] - device * key_dev, 1), :] for h in range(each)
    ]
    report[...] = jnp.concatenate(lines, axis=0).astype(BF16)


def all_barrier(gx, gy, me_x, me_y):
    barrier = pltpu.get_barrier_semaphore()
    device = me_x * gy + me_y
    devices = gx * gy

    @pl.loop(1, devices)
    def _(step):
        other = lax.rem(device + step, devices)
        target = (other // gy, lax.rem(other, gy))
        pl.semaphore_signal(barrier, inc=1, device_id=target, device_id_type=MESH)

    pl.semaphore_wait(barrier, devices - 1)


def exchange(me, count, moves, address):
    for source, landing, send_sem, recv_sem, local_sem in moves:
        pltpu.make_async_copy(source(me), landing(me), local_sem).start()

    def remote(other, move):
        source, landing, send_sem, recv_sem, local_sem = move
        return pltpu.make_async_remote_copy(
            src_ref=source(other),
            dst_ref=landing(me),
            send_sem=send_sem.at[other],
            recv_sem=recv_sem.at[me],
            device_id=address(other),
            device_id_type=MESH,
        )

    def finish(other, move):
        source, landing, send_sem, recv_sem, local_sem = move
        copy = pltpu.make_async_remote_copy(
            src_ref=source(other),
            dst_ref=landing(other),
            send_sem=send_sem.at[other],
            recv_sem=recv_sem.at[other],
            device_id=address(other),
            device_id_type=MESH,
        )
        copy.wait_send()
        copy.wait_recv()

    @pl.loop(1, count)
    def _(step):
        for move in moves:
            remote(lax.rem(me + step, count), move).start()

    def end():
        @pl.loop(1, count)
        def _(step):
            for move in moves:
                finish(lax.rem(me + step, count), move)

        for source, landing, send_sem, recv_sem, local_sem in moves:
            pltpu.make_async_copy(source(me), landing(me), local_sem).wait()

    return end


def to_owners(gx, gy, send, tally, small, got, got_tally, got_small, sem_a, sem_b, sem_c, sem_d, sem_e, sem_f, local):
    me_x, me_y = lax.axis_index("gx"), lax.axis_index("gy")
    all_barrier(gx, gy, me_x, me_y)
    rows = (lambda i: send.at[i], lambda i: got.at[i], sem_a, sem_b, local.at[0])
    tallies = (lambda i: tally.at[i], lambda i: got_tally.at[i], sem_c, sem_d, local.at[1])
    end_x = exchange(me_x, gx, [rows, tallies], lambda i: (i, me_y))
    others = (lambda i: small.at[i], lambda i: got_small.at[i], sem_e, sem_f, local.at[2])
    end_all = exchange(
        me_x * gy + me_y, gx * gy, [others], lambda i: (i // gy, lax.rem(i, gy))
    )
    end_x()
    end_all()


def to_ranges(gx, gy, send, scales, tally, got, got_scales, got_tally, sem_a, sem_b, sem_c, sem_d, sem_e, sem_f, local):
    me_x, me_y = lax.axis_index("gx"), lax.axis_index("gy")
    all_barrier(gx, gy, me_x, me_y)
    rows = (
        lambda i: send.at[lax.rem(i, gy) * gx + i // gy],
        lambda i: got.at[i],
        sem_a,
        sem_b,
        local.at[0],
    )
    factors = (
        lambda i: scales.at[lax.rem(i, gy) * gx + i // gy],
        lambda i: got_scales.at[i],
        sem_e,
        sem_f,
        local.at[2],
    )
    end_all = exchange(
        me_x * gy + me_y, gx * gy, [rows, factors], lambda i: (i // gy, lax.rem(i, gy))
    )
    tallies = (lambda i: tally.at[i], lambda i: got_tally.at[i], sem_c, sem_d, local.at[1])
    end_y = exchange(me_y, gy, [tallies], lambda i: (me_x, i))
    end_y()
    end_all()


def shaped(*dims, dtype=F32):
    return jax.ShapeDtypeStruct(dims, dtype)


def split_body(measures, row_keys, orders, heavy_keys, key_slot):
    rows, columns = measures.shape
    gx, gy = lax.axis_size("gx"), lax.axis_size("gy")
    devices = gx * gy
    key_dev = orders.shape[0]
    key_rows = key_dev // LANES
    own = key_dev * gy
    nr = key_slot.shape[0] // LANES
    heavy = heavy_keys.shape[0]
    each = heavy // devices
    capacity = max(rows // 32, 3 * rows // (4 * gx)) // 4
    segments = gx * capacity
    cfg = dict(
        rows=rows,
        block=min(rows, 2048),
        nr=nr,
        gx=gx,
        gy=gy,
        devices=devices,
        own=own,
        kpp=key_dev // gx,
        key_rows=key_rows,
        heavy=heavy,
        heavy_each=each,
        height=-(-(each + key_rows) // 8) * 8,
        capacity=capacity,
        segments=segments,
        seg_block=512 if segments % 512 == 0 else segments,
    )
    height = cfg["height"]
    group = own // LANES
    params = pltpu.CompilerParams(vmem_limit_bytes=LIMIT)
    table = key_slot.reshape(nr, LANES)
    kpp = cfg["kpp"]
    tall = group + -(-len(pieces(capacity)) // 8) * 8
    send, tally, small = pl.pallas_call(
        functools.partial(gather_rows, cfg),
        out_shape=(
            shaped(gx, capacity, columns, dtype=jnp.int16),
            shaped(gx, tall, LANES),
            shaped(devices * height, LANES),
        ),
        in_specs=[VMEM] * 4,
        out_specs=(VMEM,) * 3,
        scratch_shapes=[pltpu.VMEM((1, rows), jnp.int32), pltpu.VMEM((segments, columns), F32)],
        compiler_params=params,
    )(measures, row_keys.reshape(1, rows), heavy_keys.reshape(heavy, 1), table)
    dma = pltpu.SemaphoreType.DMA
    got, got_tally, got_small = pl.pallas_call(
        functools.partial(to_owners, gx, gy),
        out_shape=(
            shaped(gx, capacity, columns, dtype=jnp.int16),
            shaped(gx, tall, LANES),
            shaped(devices, height, LANES),
        ),
        in_specs=[ANY] * 3,
        out_specs=(ANY,) * 3,
        scratch_shapes=[dma((gx,))] * 4 + [dma((devices,))] * 2 + [dma((3,))],
        compiler_params=pltpu.CompilerParams(collective_id=0, has_side_effects=True),
    )(send, tally, small.reshape(devices, height, LANES))
    send2, scales2, tally2 = pl.pallas_call(
        functools.partial(place_rows, cfg),
        out_shape=(
            shaped(devices, kpp, columns, dtype=jnp.int16),
            shaped(devices, 1, LANES),
            shaped(group, LANES),
        ),
        in_specs=[VMEM] * 3,
        out_specs=(VMEM,) * 3,
        scratch_shapes=[pltpu.VMEM((own, LANES), F32), pltpu.VMEM((gx * group, LANES), F32)],
        compiler_params=params,
    )(got, got_tally, table)
    got2, got_scales2, got_tally2 = pl.pallas_call(
        functools.partial(to_ranges, gx, gy),
        out_shape=(
            shaped(devices, kpp, columns, dtype=jnp.int16),
            shaped(devices, 1, LANES),
            shaped(gy, key_rows, LANES),
        ),
        in_specs=[ANY] * 3,
        out_specs=(ANY,) * 3,
        scratch_shapes=[dma((devices,))] * 2
        + [dma((gy,))] * 2
        + [dma((devices,))] * 2
        + [dma((3,))],
        compiler_params=pltpu.CompilerParams(collective_id=1, has_side_effects=True),
    )(send2, scales2, tally2.reshape(gy, key_rows, LANES))
    result, report, slot_rows = pl.pallas_call(
        functools.partial(join_rows, cfg),
        out_shape=(
            shaped(key_dev, columns, dtype=BF16),
            shaped(each, columns, dtype=BF16),
            shaped(key_rows, LANES),
        ),
        in_specs=[SMEM] + [VMEM] * 6,
        out_specs=(VMEM,) * 3,
        scratch_shapes=[pltpu.VMEM((key_dev, LANES), F32)] * 2,
        compiler_params=params,
    )(
        heavy_keys,
        got2,
        got_scales2,
        got_small.reshape(devices * height, LANES),
        got_tally2.reshape(gy * key_rows, LANES),
        orders,
        table,
    )
    return (result, report, slot_rows.reshape(key_dev))


def fused(
    cfg, measures, keys_hbm, heavy_hbm, table_hbm,
    got2, scales2, hgot, side_out,
    keys, heavy, table, side, rows_in, pair, parity, seg_hot, group_row, local_row, hist, hist16, send1, got1, goth, cnt_got,
    codes, ranks, found, wide, hsend, send2, srow, tsend, tgot,
    load_sem, in_sem, out_sem, back_sem, row_sem, own_sem,
):
    gx, gy, nr, rows, block = cfg["gx"], cfg["gy"], cfg["nr"], cfg["rows"], cfg["block"]
    devices, own, kpp, key_rows = cfg["devices"], cfg["own"], cfg["kpp"], cfg["key_rows"]
    cap, extra, seg, deep = cfg["cap"], cfg["extra"], cfg["seg"], cfg["deep"]
    each, planes, half_seg = cfg["each"], cfg["planes"], cfg["seg"] // 2
    used, at_once = (cap + extra) // 2, cfg["at_once"]
    key_dev = key_rows * LANES
    per_tile = LANES // kpp
    mx, my = lax.axis_index("gx"), lax.axis_index("gy")
    me = mx * gy + my
    z, j = me // gx, lax.rem(me, gx)

    def remote(src, dst, send_sem, recv_sem, where):
        return pltpu.make_async_remote_copy(
            src_ref=src, dst_ref=dst, send_sem=send_sem, recv_sem=recv_sem,
            device_id=where, device_id_type=MESH,
        )

    def in_plane(p, x):
        d = p * gx + x
        return (d // gy, lax.rem(d, gy))

    beside = [lax.rem(my + s, gy) for s in range(gy)]

    def every_other(act):
        for y in beside[1:]:
            act(mx * gy + y, (mx, y))

        @pl.loop(1, gx)
        def _(s):
            x = lax.rem(mx + s, gx)
            for y in beside:
                act(x * gy + y, (x, y))

    self_id = (mx, my)
    others = devices - 1
    COUNTS, HISTS, ROWS, MERGED, SCALES, HEADS, TOTALS = range(7)

    loads = [
        pltpu.make_async_copy(source, target, in_sem.at[i])
        for i, (source, target) in enumerate(
            [(keys_hbm, keys), (heavy_hbm, heavy), (table_hbm, table)]
        )
    ]
    for one in loads:
        one.start()
    load = pltpu.make_async_copy(measures, rows_in, load_sem)
    load.start()

    steps_to = sorted(range(1, gx), key=lambda m: (-bin(m >> 1).count("1"), m & 1, -m)) + [0]
    partner = []
    for m in steps_to:
        x, bit = j, 1
        while bit < gx:
            if m & bit:
                x = x + bit * (1 - 2 * lax.rem(x // bit, 2))
            bit *= 2
        partner.append(x)

    barrier = pltpu.get_barrier_semaphore()

    every_other(
        lambda d, where: pl.semaphore_signal(
            barrier, inc=1, device_id=where, device_id_type=MESH
        )
    )
    for one in loads:
        one.wait()

    chains = [jnp.zeros((nr, LANES), F32)] * 2
    for c in range(rows // block):
        span = slice(c * block, (c + 1) * block)
        key = keys[:, span]
        row_hot = onehot(iota((nr, block), 0) == key >> 7)
        seg_hot[:, span] = row_hot
        column_hot = onehot(iota((LANES, block), 0) == (key & 127))
        chains[c % 2] = chains[c % 2] + dot(row_hot, column_hot, NT)
    total = joined_chains(chains)
    hist[...] = total.reshape(devices, key_rows, LANES)
    hist16[...] = total.astype(jnp.int32).astype(jnp.int16)
    cnt_got[me] = hist[me]

    owner = table[...] // own
    heavy_key = heavy[...]
    heads = heavy_key.shape[1]
    code = iota((1, heads), 1) + 1
    row_of = iota((nr, heads), 0) == heavy_key >> 7
    col_of = onehot(iota((LANES, heads), 0) == (heavy_key & 127))
    low = dot(jnp.where(row_of, (code & 127).astype(F32), 0.0).astype(BF16), col_of, NT)
    high = dot(jnp.where(row_of, (code >> 7).astype(F32), 0.0).astype(BF16), col_of, NT)
    which = (low + 128.0 * high).astype(jnp.int32)
    codes[...] = which.astype(F32).reshape(devices, key_rows, LANES)
    light = which == 0
    present = (total > 0.0) & light
    lane_r, lane_c = iota((LANES, 2 * LANES), 0), iota((LANES, 2 * LANES), 1)
    upper = onehot((lane_c >= LANES) | (lane_r < lane_c))
    lower = onehot(iota((nr, nr), 1) < iota((nr, nr), 0))
    flags = jnp.concatenate(
        [jnp.where(present & (owner == x), 1.0, 0.0) for x in range(gx)], axis=0
    ).astype(BF16)
    both = dot(flags, upper)
    local = jnp.zeros((nr, LANES), F32)
    for x in range(gx):
        part = both[x * nr : (x + 1) * nr]
        rank = part[:, :LANES] + dot(lower, part[:, LANES:].astype(BF16))
        local = local + jnp.where(owner == x, rank, 0.0)
    head = which - 1
    block_of = head // each
    group = jnp.where(light, owner, lax.rem(block_of, gx))
    local = jnp.where(
        light, local, (cap + (block_of // gx) * each + lax.rem(head, each)).astype(F32)
    )
    tables = jnp.concatenate([256.0 * group.astype(F32).T, local.T], axis=1).astype(BF16)
    pl.semaphore_wait(barrier, devices - 1)

    for s in range(gx - 1):
        remote(
            hist16, goth.at[s], out_sem.at[HISTS], back_sem.at[HISTS], in_plane(z, partner[s])
        ).start()
    every_other(
        lambda d, where: remote(
            hist.at[d], cnt_got.at[me], out_sem.at[COUNTS], back_sem.at[COUNTS], where
        ).start()
    )

    load.wait()
    for c in range(rows // min(block, 512)):
        block = min(cfg["block"], 512)
        span = slice(c * block, (c + 1) * block)
        row_hot = seg_hot[:, span]
        spread = dot(tables, jnp.concatenate([row_hot, row_hot], axis=0))
        mask = iota((LANES, block), 0) == (keys[:, span] & 127)
        both = jnp.sum(jnp.where(mask, spread, 0.0), axis=0, keepdims=True).astype(jnp.int32)
        group_row[:, span] = both >> 8
        inside = both & 255
        local_row[:, span] = inside >> 1
        odd = (inside & 1).astype(F32)
        for i in range(block // LANES):
            at = c * (block // LANES) + i
            parity[at : at + 1, :] = odd[:, i * LANES : (i + 1) * LANES]

    block = cfg["block"]
    turned = parity[...].T

    def halves(c):
        span = slice(c * LANES, (c + 1) * LANES)
        line = rows_in[span, :]
        odd = line * jnp.broadcast_to(turned[:, c : c + 1], (LANES, LANES)).astype(BF16)
        pair[span, LANES:] = odd
        pair[span, :LANES] = line - odd

    def encode(values):
        largest = jnp.max(jnp.abs(values), axis=1, keepdims=True)
        power = jnp.floor(jnp.log2(jnp.maximum(largest, 1e-30))) + 1.0
        fixed = jnp.clip(jnp.round(values * jnp.exp2(15.0 - power)), -32767.0, 32767.0)
        return fixed, power

    for first in range(0, gx, at_once):
        steps = range(first, first + at_once)
        chains = [jnp.zeros((at_once * half_seg, 2 * LANES), F32)] * 2
        for c in range(rows // block):
            span = slice(c * block, (c + 1) * block)
            group, local = group_row[:, span], local_row[:, span]
            if first == 0:
                for i in range(c * block // LANES, (c + 1) * block // LANES):
                    halves(i)
            hot = [
                jnp.where(
                    iota((half_seg, block), 0)
                    == jnp.where(group == partner[s], local, -1),
                    1.0,
                    0.0,
                )
                for s in steps
            ]
            chains[c % 2] = chains[c % 2] + dot(
                jnp.concatenate(hot, axis=0).astype(BF16), pair[span, :]
            )
        acc = joined_chains(chains)
        for s in steps:
            at = (s - first) * half_seg
            both = acc[at : at + half_seg]
            fixed, power = encode(jnp.concatenate([both[:, :LANES], both[:, LANES:]], axis=0))
            lines = []
            for top, size in pieces(seg):
                diagonal = iota((size, LANES), 0) == iota((size, LANES), 1)
                lines.append(
                    jnp.sum(jnp.where(diagonal, power[top : top + size], 0.0), axis=0, keepdims=True)
                )
            foot = jnp.zeros((half_seg - used, LANES), F32)
            for n, one in enumerate(lines):
                foot = jnp.where(iota(foot.shape, 0) == n, one, foot)
            whole = jnp.concatenate([fixed[:used], foot, fixed[half_seg:]], axis=0)
            send1[s] = whole.astype(jnp.int32).astype(jnp.int16)
            if s < gx - 1:
                remote(
                    send1.at[s], got1.at[s], out_sem.at[ROWS], row_sem.at[s],
                    in_plane(z, partner[s]),
                ).start()

    def all_of(ref, kind, number):
        return remote(
            ref.at[0:number], ref.at[0:number], out_sem.at[kind], back_sem.at[kind], self_id
        )

    all_of(goth, HISTS, gx - 1).wait_recv()
    mine = (owner == j) & light
    arrived = []
    for t in range(gx):
        here = hist16[...] if t == gx - 1 else goth[t]
        arrived.append(jnp.where((here.astype(jnp.int32) > 0) & mine, 1.0, 0.0))
    flags = jnp.concatenate(arrived, axis=0)
    both = dot(flags.astype(BF16), upper)
    for t in range(gx):
        part = both[t * nr : (t + 1) * nr]
        rank = (part[:, :LANES] + dot(lower, part[:, LANES:].astype(BF16))).astype(jnp.int32)
        rank = ((rank >> 1) + (rank & 1) * half_seg + 1).astype(F32)
        ranks[t * nr : (t + 1) * nr, :] = rank * flags[t * nr : (t + 1) * nr]
    own_flags = onehot(owner == j)
    both = dot(own_flags, upper)
    row_r, row_c = iota((nr, nr), 0), iota((nr, nr), 1)
    near = onehot((row_c < row_r) & (row_r // key_rows == row_c // key_rows))
    rank = both[:, :LANES] + dot(near, both[:, LANES:].astype(BF16))
    rank = jnp.where(owner == j, rank, -1.0).astype(jnp.int32)
    for d in range(devices):
        hot, tall = [], []
        for q in range(key_rows):
            r = d * key_rows + q
            hot.append(onehot(iota((kpp, LANES), 0) == rank[r : r + 1]))
            tall.append(ranks[pl.ds(r, gx, stride=nr), :].astype(BF16))
        found[d * kpp : (d + 1) * kpp, 0:gx] = dot(
            jnp.concatenate(hot, axis=1), jnp.concatenate(tall, axis=1), NT
        )

    all_of(cnt_got, COUNTS, others).wait()

    counted = cnt_got[0]
    for d in range(1, devices):
        counted = counted + cnt_got[d]
    side[key_rows : 2 * key_rows, :] = counted
    tsend[...] = jnp.where(codes[me] == 0.0, counted, 0.0)
    tgot[mx] = tsend[...]

    @pl.loop(1, gx)
    def _(s):
        x = lax.rem(mx + s, gx)
        remote(tsend, tgot.at[mx], out_sem.at[TOTALS], back_sem.at[TOTALS], (x, my)).start()

    heads_sum = [jnp.zeros((extra // 2, LANES), F32)] * 2
    powers = []
    for t in range(gx):
        if t < gx - 1:
            remote(send1.at[t], got1.at[t], out_sem.at[ROWS], row_sem.at[t], self_id).wait_recv()
            block16 = got1[t]
        else:
            block16 = send1[t]
        value = block16.astype(jnp.int32)
        wide[t, 0:seg, :LANES] = (value >> 8).astype(F32).astype(BF16)
        wide[t, 0:seg, LANES:] = (value & 255).astype(F32).astype(BF16)
        if deep > seg:
            wide[t, seg:deep, :] = jnp.zeros((deep - seg, 2 * LANES), BF16)
        scale = jnp.exp2(value[used : used + len(pieces(seg))].astype(F32) - 15.0)
        powers.append(
            jnp.concatenate([scale[p : p + 1] for p in range(deep // LANES)], axis=1)
        )
        for b in range(2):
            top = b * half_seg + cap // 2
            p, at = top // LANES, top % LANES
            column = jnp.sum(
                jnp.where(
                    iota((extra // 2, LANES), 1) == iota((extra // 2, LANES), 0) + at,
                    scale[p : p + 1],
                    0.0,
                ),
                axis=1, keepdims=True,
            )
            heads_sum[b] = heads_sum[b] + value[top : top + extra // 2].astype(F32) * column
    hsend[...] = jnp.concatenate(heads_sum, axis=0)

    local_heads = pltpu.make_async_copy(hsend, hgot.at[z], own_sem.at[0])
    local_heads.start()

    @pl.loop(1, planes)
    def _(s):
        other = lax.rem(z + s, planes)
        remote(
            hsend, hgot.at[z], out_sem.at[HEADS], back_sem.at[HEADS], in_plane(other, j)
        ).start()

    chunk = gx * kpp
    shift = lax.rem(j, per_tile) * kpp
    half = planes // 2
    lanes = (iota((1, deep), 1) + 1).astype(F32)
    if planes == 4:
        order = [
            lax.rem(z + half, planes), planes - 1 - z,
            planes - 1 - lax.rem(z + half, planes), z,
        ]
    else:
        order = [lax.rem(z + s, planes) for s in range(1, planes + 1)]
    diagonal = iota((kpp, LANES), 1) == iota((kpp, LANES), 0) + shift
    wave = gx // 2
    part = wave * kpp
    for c in range(planes):
        far, last = order[c], c == planes - 1
        for first in range(0, gx, wave):
            top = pl.multiple_of(far * chunk + first * kpp, part)
            spot = found[pl.ds(top, part), :]
            chains = [jnp.zeros((part, 2 * LANES), F32)] * 2
            for t in range(gx):
                hit = spot[:, t : t + 1] == lanes
                chains[t % 2] = chains[t % 2] + dot(
                    jnp.where(hit, powers[t], 0.0).astype(BF16), wide[t]
                )
            acc = joined_chains(chains)
            fixed, power = encode(acc[:, :LANES] * 256.0 + acc[:, LANES:])
            send2[c, first : first + wave] = (
                fixed.astype(jnp.int32).astype(jnp.int16).reshape(wave, kpp, LANES)
            )
            scale = jnp.exp2(power - 15.0)
            for x in range(wave):
                srow[c, first + x] = jnp.sum(
                    jnp.where(diagonal, scale[x * kpp : (x + 1) * kpp], 0.0), axis=0, keepdims=True
                ).astype(BF16)

            def one_block(x, c=c, far=far):
                where = in_plane(far, x)
                remote(
                    send2.at[c, x], got2.at[me], out_sem.at[MERGED], back_sem.at[MERGED], where
                ).start()
                remote(
                    srow.at[c, x], scales2.at[me], out_sem.at[SCALES], back_sem.at[SCALES], where
                ).start()

            @pl.loop(0, wave)
            def _(s, first=first, last=last, one_block=one_block):
                x = first + lax.rem(j + s, wave)
                if last:
                    pl.when(x != j)(lambda: one_block(x))
                else:
                    one_block(x)

    keep = pltpu.make_async_copy(send2.at[planes - 1, j], got2.at[me], own_sem.at[1])
    keep.start()
    keep_row = pltpu.make_async_copy(srow.at[planes - 1, j], scales2.at[me], own_sem.at[2])
    keep_row.start()

    all_of(tgot, TOTALS, gx - 1).wait()

    base = me * key_dev
    left, right = [], []
    for m in range(gx):
        slots = table[pl.ds((m * gy + my) * key_rows, key_rows), :] - base
        for q in range(key_rows):
            line = slots[q : q + 1]
            amount = tgot[m, q : q + 1, :].astype(jnp.int32)
            bands = [
                jnp.where(
                    iota((8, LANES), 0) == (line >> 7), ((amount >> (8 * b)) & 255).astype(F32), 0.0
                )
                for b in range(3)
            ]
            left.append(jnp.concatenate(bands + [jnp.zeros((8, LANES), F32)], axis=0).astype(BF16))
            right.append(onehot(iota((LANES, LANES), 0) == (line & 127)))
    middle = len(left) // 2
    bands = joined_chains(
        [
            dot(jnp.concatenate(left[part], axis=1), jnp.concatenate(right[part], axis=1), NT)
            for part in (slice(0, middle), slice(middle, None))
        ]
    )
    side[2 * key_rows : 3 * key_rows, :] = (
        bands[0:8] + 256.0 * bands[8:16] + 65536.0 * bands[16:24]
    )[0:key_rows]
    owner = table[pl.ds(me * key_rows, key_rows), :] // own
    flags = jnp.concatenate([jnp.where(owner == x, 1.0, 0.0) for x in range(gx)], axis=0)
    rank = group_rank(flags.astype(BF16), key_rows)
    place = jnp.zeros((key_rows, LANES), F32)
    for x in range(gx):
        inside = rank[x * key_rows : (x + 1) * key_rows] + float(x * kpp)
        place = place + jnp.where(owner == x, inside, 0.0)
    side[0:key_rows, :] = place
    side[3 * key_rows : 4 * key_rows, :] = codes[me] - (each * me).astype(F32)
    hand_over = pltpu.make_async_copy(side, side_out, own_sem.at[3])
    hand_over.start()

    all_of(goth, HISTS, gx - 1).wait_send()
    all_of(send1, ROWS, gx - 1).wait_send()
    local_heads.wait()
    keep.wait()
    keep_row.wait()
    hand_over.wait()
    all_of(hgot, HEADS, planes - 1).wait()
    all_of(got2, MERGED, others).wait()
    all_of(scales2, SCALES, others).wait()


def join(
    cfg, got_hbm, scales_hbm, heads_hbm, side_hbm, orders_hbm, result, report, slot_rows,
    got, scales, heads, side, orders, done, lines_out, sems, out_sems,
):
    gx, gy, kpp = cfg["gx"], cfg["gy"], cfg["kpp"]
    key_rows, each, planes, extra = cfg["key_rows"], cfg["each"], cfg["planes"], cfg["extra"]
    key_dev = key_rows * LANES
    per_tile = LANES // kpp
    loads = [
        pltpu.make_async_copy(got_hbm.at[p * gx : (p + 1) * gx], got.at[p], sems.at[4 + p])
        for p in range(planes)
    ]
    tables = [
        pltpu.make_async_copy(source, target, sems.at[i])
        for i, (source, target) in enumerate(
            [(side_hbm, side), (scales_hbm, scales), (heads_hbm, heads), (orders_hbm, orders)]
        )
    ]
    for one in tables[:2] + loads + tables[2:]:
        one.start()
    z = (lax.axis_index("gx") * gy + lax.axis_index("gy")) // gx
    tables[0].wait()
    tables[1].wait()
    columns = side[...].T
    stores = [
        pltpu.make_async_copy(
            side.at[2 * key_rows : 3 * key_rows, :], slot_rows, out_sems.at[key_rows]
        )
    ]
    stores[0].start()
    lines = []
    for p in range(planes):
        tiles = []
        for x in range(0, gx, per_tile):
            tile = scales[p * gx + x].astype(F32)
            for i in range(1, per_tile):
                tile = tile + scales[p * gx + x + i].astype(F32)
            tiles.append(tile)
        lines.append(jnp.concatenate(tiles, axis=1))
    tables[2].wait()
    tables[3].wait()
    small = heads[0]
    for p in range(1, planes):
        small = small + heads[p]
    own_lines = []
    for h in range(each):
        entry = z * each + h
        spot = lax.rem(entry, 2) * (extra // 2) + entry // 2
        own_lines.append(
            jnp.sum(jnp.where(iota((extra, LANES), 0) == spot, small, 0.0), axis=0, keepdims=True)
        )
    values = []
    for p in range(planes):
        loads[p].wait()
        value = got[p].reshape(key_dev, LANES).astype(jnp.int32)
        values.append(
            jnp.concatenate([(value >> 8).astype(F32), (value & 255).astype(F32)], axis=1).astype(BF16)
        )
    picked = [jnp.zeros((1, LANES), F32)] * each
    for q in range(key_rows):
        at = slice(q * LANES, (q + 1) * LANES)
        hit = columns[:, q : q + 1] == iota((LANES, key_dev), 1).astype(F32)
        chains = [jnp.zeros((LANES, 2 * LANES), F32)] * 2
        for p in range(planes):
            chains[p % 2] = chains[p % 2] + dot(
                jnp.where(hit, lines[p], 0.0).astype(BF16), values[p]
            )
        both = joined_chains(chains)
        sums = both[:, :LANES] * 256.0 + both[:, LANES:]
        head = columns[:, 3 * key_rows + q : 3 * key_rows + q + 1]
        for h in range(each):
            sums = sums + jnp.where(head == float(h + 1), own_lines[h], 0.0)
        scale = lax.rsqrt(1.0 + columns[:, key_rows + q : key_rows + q + 1])
        value = orders[at, :].astype(F32) * sums * scale
        for h in range(each):
            picked[h] = picked[h] + jnp.sum(
                jnp.where(head == float(h + 1), value, 0.0), axis=0, keepdims=True
            )
        done[at, :] = value.astype(BF16)
        stores.append(pltpu.make_async_copy(done.at[at, :], result.at[at, :], out_sems.at[q]))
        stores[-1].start()
    lines_out[...] = jnp.concatenate(picked, axis=0).astype(BF16)
    stores.append(pltpu.make_async_copy(lines_out, report, out_sems.at[key_rows + 1]))
    stores[-1].start()
    for one in stores:
        one.wait()


def body(measures, row_keys, orders, heavy_keys, key_slot):
    rows, columns = measures.shape
    gx, gy = lax.axis_size("gx"), lax.axis_size("gy")
    devices = gx * gy
    key_dev = orders.shape[0]
    key_rows = key_dev // LANES
    nr = key_slot.shape[0] // LANES
    heavy = heavy_keys.shape[0]
    each = heavy // devices
    if gx * nr > 2048 or gx & (gx - 1):
        return split_body(measures, row_keys, orders, heavy_keys, key_slot)
    planes = devices // gx
    cap = max(rows // 32, 3 * rows // (4 * gx)) // 4
    extra = planes * each
    seg = 2 * (-(-((cap + extra) // 2 + len(pieces(cap + extra + 16))) // 8) * 8)
    deep = -(-cap // LANES) * LANES
    kpp = key_dev // gx
    cfg = dict(
        rows=rows, block=min(rows, 2048), nr=nr, gx=gx, gy=gy, devices=devices,
        own=key_dev * gy, kpp=kpp, key_rows=key_rows, each=each, planes=planes,
        cap=cap, extra=extra, seg=seg, at_once=2 if gx % 2 == 0 else gx, deep=max(deep, -(-seg // LANES) * LANES),
    )
    deep = cfg["deep"]
    table = key_slot.reshape(nr, LANES)
    dma = pltpu.SemaphoreType.DMA
    i16 = jnp.int16
    got, scales, heads, side = pl.pallas_call(
        functools.partial(fused, cfg),
        out_shape=(
            shaped(devices, kpp, columns, dtype=i16),
            shaped(devices, 1, LANES, dtype=BF16),
            shaped(planes, extra, LANES),
            shaped(4 * key_rows, LANES),
        ),
        in_specs=[ANY] * 4,
        out_specs=(ANY,) * 4,
        scratch_shapes=[
            pltpu.VMEM((1, rows), jnp.int32),
            pltpu.VMEM((1, heavy), jnp.int32),
            pltpu.VMEM((nr, LANES), jnp.int32),
            pltpu.VMEM((4 * key_rows, LANES), F32),
            pltpu.VMEM((rows, columns), BF16),
            pltpu.VMEM((rows, 2 * columns), BF16),
            pltpu.VMEM((rows // LANES, LANES), F32),
            pltpu.VMEM((nr, rows), BF16),
            pltpu.VMEM((1, rows), jnp.int32),
            pltpu.VMEM((1, rows), jnp.int32),
            pltpu.VMEM((devices, key_rows, LANES), F32),
            pltpu.VMEM((nr, LANES), i16),
            pltpu.VMEM((gx, seg, LANES), i16),
            pltpu.VMEM((gx, seg, LANES), i16),
            pltpu.VMEM((gx, nr, LANES), i16),
            pltpu.VMEM((devices, key_rows, LANES), F32),
            pltpu.VMEM((devices, key_rows, LANES), F32),
            pltpu.VMEM((gx * nr, LANES), F32),
            pltpu.VMEM((devices * kpp, LANES), F32),
            pltpu.VMEM((gx, deep, 2 * LANES), BF16),
            pltpu.VMEM((extra, LANES), F32),
            pltpu.VMEM((planes, gx, kpp, LANES), i16),
            pltpu.VMEM((planes, gx, 1, LANES), BF16),
            pltpu.VMEM((key_rows, LANES), F32),
            pltpu.VMEM((gx, key_rows, LANES), F32),
            dma,
            dma((3,)),
            dma((7,)),
            dma((7,)),
            dma((gx,)),
            dma((4,)),
        ],
        compiler_params=pltpu.CompilerParams(
            collective_id=2, has_side_effects=True, vmem_limit_bytes=LIMIT
        ),
    )(measures, row_keys.reshape(1, rows), heavy_keys.reshape(1, heavy), table)
    result, report, slot_rows = pl.pallas_call(
        functools.partial(join, cfg),
        out_shape=(
            shaped(key_dev, columns, dtype=BF16),
            shaped(each, columns, dtype=BF16),
            shaped(key_rows, LANES),
        ),
        in_specs=[ANY] * 5,
        out_specs=(ANY,) * 3,
        scratch_shapes=[
            pltpu.VMEM((planes, gx, kpp, columns), i16),
            pltpu.VMEM((devices, 1, LANES), BF16),
            pltpu.VMEM((planes, extra, LANES), F32),
            pltpu.VMEM((4 * key_rows, LANES), F32),
            pltpu.VMEM((key_dev, columns), BF16),
            pltpu.VMEM((key_dev, columns), BF16),
            pltpu.VMEM((each, columns), BF16),
            dma((4 + planes,)),
            dma((key_rows + 2,)),
        ],
        compiler_params=pltpu.CompilerParams(vmem_limit_bytes=LIMIT),
    )(got, scales, heads, side, orders)
    return (result, report, slot_rows.reshape(key_dev))


def solution(mesh):
    return jax.shard_map(
        body,
        mesh=mesh,
        in_specs=(P(("gx", "gy"), None), P(("gx", "gy")), P(("gx", "gy"), None), P(), P()),
        out_specs=(P(("gx", "gy"), None), P(("gx", "gy"), None), P(("gx", "gy"))),
        check_vma=False,
    )
```
